512 devices in a mesh: dp: 32 (over x, y, core), expert: 16 (over z).
Axes of the slice: x: 4, y: 4, z: 16, core: 2. Of those that a mesh axis runs over, the one named last changes fastest.
Arguments:
- tokens: bfloat16 [131072, 1024], P(('dp', 'expert')), may hold values from -6 to 6
- grad_out: bfloat16 [131072, 1024], P(('dp', 'expert')), may hold values from -6 to 6
- expert_ids: int32 [131072, 8], P(('dp', 'expert')), may hold values from 0 to 127, all different within a row; in each aligned block of 256 rows (0 to 255, 256 to 511, ...) at most 32 rows name the same one
- router_weight: bfloat16 [1024, 128], replicated, may hold values from -0.1875 to 0.1875
- gate_weight_stack: bfloat16 [16, 1024, 384], P('expert'), may hold values from -0.1875 to 0.1875
- up_weight_stack: bfloat16 [16, 1024, 384], P('expert'), may hold values from -0.1875 to 0.1875
- down_weight_stack: bfloat16 [16, 384, 1024], P('expert'), may hold values from -0.3125 to 0.3125
Outputs:
- grad_tokens: bfloat16 [131072, 1024], P(('dp', 'expert'))
- grad_gate: float32 [16, 1024, 384], P('expert', 'dp')
- grad_up: float32 [16, 1024, 384], P('expert', 'dp')
- grad_down: float32 [16, 384, 1024], P('expert', 'dp')
- grad_router: float32 [1024, 128], replicated
The draws below stay inside these ranges and needn't reach their ends.
Inputs may be any that keep to these rules, and one draw needn't show every extreme that they name: `expert_ids`: each row names 8 different experts; within the rows of one device (aligned blocks of 256 rows) no expert is named by more than 32 rows.
All inputs are finite; a program needn't handle non-finite values.
Results may differ from the reference program's by a relative error of at most 0.018.
Values may be sent and summed in bfloat16 or wider, within the bound.
A program may use at most 64 MiB of HBM per device.

```python
import math
import jax
import jax.numpy as jnp
import numpy as np
from jax import lax

D = 1024
FF = 384
EXPERTS = 128
TOP = 8
FLIGHT = 1
TOK_DEV = 256
CAP = 32
NFL = 16
TOKENS = 131072
N_DP = 32
N_EXPERT = 16


def levels(key, extent, pieces, least, largest):
    factor_of = 1.0
    for axis_at, shards_of in pieces:
        heights = jax.random.uniform(jax.random.fold_in(jax.random.fold_in(key, 6), axis_at), (shards_of,), jnp.float32, least / len(pieces), largest / len(pieces))
        factor_of = factor_of * jnp.repeat(jnp.exp(heights), extent[axis_at] // shards_of).reshape((-1,) + (1,) * (len(extent) - 1 - axis_at))
    return factor_of


def assign_block(stream_key, own, number, rows, number_of, top, limit, skew):
    sequence = jax.random.permutation(stream_key, number_of)
    crowded, common = shares(number_of, rows * top, limit, skew, True), shares(number_of, rows * top, limit, skew, False)
    places = jnp.arange(number_of)

    def named(tallies, turn):
        used = int((tallies > 0).sum())
        fixed = max(1, used // 4)
        passed = fixed + (places - fixed + turn * (used - fixed)) % max(1, number_of - fixed)
        return jnp.zeros((number_of,), jnp.int32).at[sequence[jnp.where(places < fixed, places, passed)]].set(jnp.asarray(tallies, jnp.int32))

    tallies = jnp.where(number % 4 == 0, named(crowded, number // 4), named(common, number - number // 4 - 1))
    mixed = jax.random.permutation(jax.random.fold_in(own, 3), number_of)
    donor, taker = mixed[0:number_of // 2 * 2:2], mixed[1:number_of // 2 * 2:2]
    margin = jnp.minimum(tallies[donor] - 1, limit - tallies[taker]) // 2
    margin = jnp.where((donor == sequence[0]) | (taker == sequence[0]) | (tallies[taker] == 0), 0, jnp.maximum(margin, 0))
    passed = jax.random.randint(jax.random.fold_in(own, 4), (number_of // 2,), 0, 1 << 20) % (margin + 1)
    tallies = tallies.at[donor].add(-passed).at[taker].add(passed)
    items = jnp.searchsorted(jnp.cumsum(tallies), jnp.arange(rows * top), side="right").astype(jnp.int32)
    grid = items.reshape(top, rows).T
    grid = grid[jax.random.permutation(jax.random.fold_in(own, 1), rows)]
    turn = jax.random.randint(jax.random.fold_in(own, 2), (rows, 1), 0, top)
    return jnp.take_along_axis(grid, (jnp.arange(top)[None, :] + turn) % top, axis=1)


def shares(count, total, limit, slope, full):
    portions = [(1 << 20) // math.isqrt(standing ** slope) + 1 for standing in range(1, count + 1)]
    largest = limit if full else min(limit, max(-(-total // count), total * portions[0] // sum(portions)))
    least = 1 if total - largest >= count - 1 else 0
    counts, spare = [largest] + [least] * (count - 1), total - largest - least * (count - 1)
    while spare > 0:
        movable = [i for i in range(1, count) if counts[i] < largest] or [i for i in range(1, count) if counts[i] < limit]
        pool, left = sum([portions[i] for i in movable]), spare
        for i in movable:
            extra = min(limit - counts[i], max(1, left * portions[i] // pool), spare)
            counts[i] = counts[i] + extra
            spare = spare - extra
    return np.array(counts)


def normal_values(stream_key, shape, width, limit, split=(), kind=jnp.bfloat16):
    drawn = width * jax.random.normal(stream_key, shape, jnp.float32)
    if split:
        drawn = drawn * levels(stream_key, shape, split, -0.22, 0.18)
    return jnp.clip(drawn, -limit, limit).astype(kind)


def setup_inputs(seed: int = 0) -> dict:
    seeds = jax.random.split(jax.random.key(seed), 8)
    tokens = normal_values(seeds[0], (TOKENS, D), 1.0, 6.0, ((0, 512),))
    grad_out = normal_values(seeds[1], (TOKENS, D), 1.0, 6.0, ((0, 512),))
    expert_ids_keys = jax.random.split(jax.random.fold_in(seeds[2], 1), TOKENS // TOK_DEV)
    expert_ids_turns = jax.random.permutation(jax.random.fold_in(seeds[2], 3), TOKENS // TOK_DEV)
    expert_ids = jax.vmap(lambda own, number: assign_block(jax.random.fold_in(seeds[2], 2), own, number, TOK_DEV, EXPERTS, TOP, CAP, 2))(expert_ids_keys, expert_ids_turns).reshape((TOKENS, TOP))
    router_weight = normal_values(seeds[3], (D, EXPERTS), D ** -0.5, 0.1875)
    gate_weight_stack = normal_values(seeds[4], (NFL, D, FF), D ** -0.5, 0.1875, ((0, 16),))
    up_weight_stack = normal_values(seeds[5], (NFL, D, FF), D ** -0.5, 0.1875, ((0, 16),))
    down_weight_stack = normal_values(seeds[6], (NFL, FF, D), FF ** -0.5, 0.3125, ((0, 16),))
    return dict(tokens=tokens, grad_out=grad_out, expert_ids=expert_ids, router_weight=router_weight, gate_weight_stack=gate_weight_stack, up_weight_stack=up_weight_stack, down_weight_stack=down_weight_stack)


def expert_backward(sel_tokens, sel_grads, sel_gates, w_gate, w_up, w_down):
    pre_gate = jnp.dot(sel_tokens, w_gate, preferred_element_type=jnp.float32)
    up_preactivation = jnp.dot(sel_tokens, w_up, preferred_element_type=jnp.float32)
    sigma = jax.nn.sigmoid(pre_gate)
    active_mask = (pre_gate * sigma * up_preactivation).astype(jnp.bfloat16)
    produced_rows = jnp.dot(active_mask, w_down, preferred_element_type=jnp.float32)
    gate_grad = jnp.sum(sel_grads.astype(jnp.float32) * produced_rows, axis=1).astype(jnp.bfloat16)
    output_gradient = (sel_gates.astype(jnp.float32)[:, None] * sel_grads.astype(jnp.float32)).astype(jnp.bfloat16)
    activation_gradient = jnp.dot(output_gradient, w_down.T, preferred_element_type=jnp.float32)
    up_gradient = (activation_gradient * pre_gate * sigma).astype(jnp.bfloat16)
    gate_preactivation_gradient = (activation_gradient * up_preactivation * sigma * (1.0 + pre_gate * (1.0 - sigma))).astype(jnp.bfloat16)
    token_grad = (jnp.dot(gate_preactivation_gradient, w_gate.T, preferred_element_type=jnp.float32)
                  + jnp.dot(up_gradient, w_up.T, preferred_element_type=jnp.float32)).astype(jnp.bfloat16)
    part_gate = jnp.dot(sel_tokens.T, gate_preactivation_gradient, preferred_element_type=jnp.float32)
    partial_up_gradient = jnp.dot(sel_tokens.T, up_gradient, preferred_element_type=jnp.float32)
    partial_down_gradient = jnp.dot(active_mask.T, output_gradient, preferred_element_type=jnp.float32)
    return token_grad, gate_grad, part_gate, partial_up_gradient, partial_down_gradient


def rounded(partial_value):
    return lax.optimization_barrier(partial_value.astype(jnp.bfloat16)).astype(jnp.float32)


def reference(tokens, grad_out, expert_ids, router_weight, gate_weight_stack, up_weight_stack, down_weight_stack):
    local_count = EXPERTS // N_EXPERT
    in_flight = FLIGHT * N_EXPERT
    block = N_EXPERT * CAP
    groups = N_DP * N_EXPERT
    per_device = TOK_DEV * TOP
    logits = jnp.dot(tokens, router_weight, preferred_element_type=jnp.float32)
    chosen = jnp.take_along_axis(logits, expert_ids, axis=1)
    raised = jnp.exp(chosen)
    gate_values = raised / jnp.sum(raised, axis=1, keepdims=True)
    sent_gate = gate_values.astype(jnp.bfloat16).reshape(-1)
    local_index = expert_ids % local_count
    target = jnp.where(local_index < FLIGHT, (expert_ids // local_count) * FLIGHT + local_index, -1)
    target = target.astype(jnp.int32).reshape(groups, per_device)
    onehot = (target[:, :, None] == jnp.arange(in_flight, dtype=jnp.int32)[None, None, :]).astype(jnp.int32)
    running = jnp.cumsum(onehot, axis=1).astype(jnp.int32)
    slot_rank = jnp.sum(onehot * (running - 1), axis=2).astype(jnp.int32)
    device = jnp.arange(groups, dtype=jnp.int32)[:, None]
    position = (((device // N_EXPERT) * in_flight + target) * N_EXPERT + device % N_EXPERT) * CAP + slot_rank
    position = jnp.where(target >= 0, position, N_DP * in_flight * block).astype(jnp.int32)
    routes = jnp.arange(TOKENS * TOP, dtype=jnp.int32)
    slot_route = jnp.full((N_DP * in_flight * block,), -1, jnp.int32)
    slot_route = slot_route.at[position.reshape(-1)].set(routes, mode="drop")
    table = jnp.transpose(slot_route.reshape(N_DP, in_flight, block), (1, 0, 2))

    def one_expert(operands):
        group_table, w_gate, w_up, w_down = operands

        def one_group(carry, group_routes):
            filled = group_routes >= 0
            safe_route = jnp.maximum(group_routes, 0)
            token_index = (safe_route // TOP).astype(jnp.int32)
            nothing = jnp.zeros((), jnp.bfloat16)
            sel_tokens = jnp.where(filled[:, None], tokens[token_index], nothing)
            sel_grads = jnp.where(filled[:, None], grad_out[token_index], nothing)
            sel_gates = jnp.where(filled, sent_gate[safe_route], nothing)
            token_grad, gate_grad, part_gate, partial_up_gradient, partial_down_gradient = expert_backward(
                sel_tokens, sel_grads, sel_gates, w_gate, w_up, w_down)
            total_gate, total_up, total_down = carry
            carry = (total_gate + rounded(part_gate), total_up + rounded(partial_up_gradient), total_down + rounded(partial_down_gradient))
            return carry, (token_grad, gate_grad)

        start = (jnp.zeros((D, FF), jnp.float32), jnp.zeros((D, FF), jnp.float32), jnp.zeros((FF, D), jnp.float32))
        carry, (token_grads, gate_grads) = lax.scan(one_group, start, group_table)
        return carry[0], carry[1], carry[2], token_grads, gate_grads

    grad_gate, grad_up, grad_down, token_grads, gate_grads = lax.map(
        one_expert, (table, gate_weight_stack, up_weight_stack, down_weight_stack))
    flat_route = table.reshape(-1)
    filled = flat_route >= 0
    token_target = jnp.where(filled, flat_route // TOP, TOKENS).astype(jnp.int32)
    expert_part = jnp.zeros((TOKENS, D), jnp.float32).at[token_target].add(
        token_grads.reshape(-1, D).astype(jnp.float32), mode="drop")
    route_target = jnp.where(filled, flat_route, TOKENS * TOP).astype(jnp.int32)
    gate_grad_all = jnp.zeros((TOKENS * TOP,), jnp.float32).at[route_target].add(
        gate_grads.reshape(-1).astype(jnp.float32), mode="drop").reshape(TOKENS, TOP)
    chosen_grad = gate_values * (gate_grad_all - jnp.sum(gate_values * gate_grad_all, axis=1, keepdims=True))
    token_rows = jnp.arange(TOKENS, dtype=jnp.int32)[:, None]
    logit_grad = jnp.zeros((TOKENS, EXPERTS), jnp.float32).at[token_rows, expert_ids].add(chosen_grad)
    logit_grad = logit_grad.astype(jnp.bfloat16)
    grad_router = jnp.dot(tokens.T, logit_grad, preferred_element_type=jnp.float32)
    grad_tokens = (expert_part + jnp.dot(logit_grad, router_weight.T, preferred_element_type=jnp.float32)).astype(jnp.bfloat16)
    return grad_tokens, grad_gate, grad_up, grad_down, grad_router
```

```python
import functools

import jax
import jax.numpy as jnp
from jax import lax
from jax.experimental import pallas as pl
from jax.experimental.pallas import tpu as pltpu
from jax.sharding import Mesh
from jax.sharding import PartitionSpec as P

AX = ("dp_0", "dp_1", "dp_2", "expert")
MESH = pl.DeviceIdType.MESH
F32, BF16 = jnp.float32, jnp.bfloat16

NZ = 16
NCHIP = 16
CAP = 32
DIST = (-3, -2, -1, 0, 1, 2, 3, 4, -4)
RELATIVE = tuple(d % NZ for d in DIST) + tuple((d + 8) % NZ for d in DIST[:7])
NP, NS = 9, 7
HOME = 3
ORDER = (7, 8, 0, 6, 1, 5, 2, 4)


def wrap(v, n):
    return lax.rem(v + n, n)


def remote(src, dst, send, recv, **where):
    return pltpu.make_async_remote_copy(
        src_ref=src,
        dst_ref=dst,
        send_sem=send,
        recv_sem=recv,
        device_id={AX["xycz".index(k)]: v for k, v in where.items()},
        device_id_type=MESH,
    )


def place():
    return tuple(lax.axis_index(a) for a in AX)


def greet(partners):
    barrier = pltpu.get_barrier_semaphore()
    for where in partners:
        pl.semaphore_signal(
            barrier,
            inc=1,
            device_id={AX["xycz".index(k)]: v for k, v in where.items()},
            device_id_type=MESH,
        )
    pl.semaphore_wait(barrier, len(partners))


def plane_partners(x, y):
    return [
        dict(x=wrap(x + dx, 4), y=wrap(y + dy, 4))
        for dx in range(4)
        for dy in range(4)
        if dx or dy
    ]


def dispatch_kernel(
    st, sg, sgt, wg, wu, wd,
    ptok, stok, pgrad, sgrad, gts, w2g, w2u, w2d,
    t_send, t_recv, g_send, g_recv, gt_send, gt_recv,
    wz_send, wz_recv, wp_send, wp_recv, wc_send, wc_recv, loc,
):
    x, y, c, z = place()
    me = x * 4 + y
    other = 1 - c
    greet(
        [dict(z=wrap(z + d, NZ)) for d in (-4, -3, -2, -1, 1, 2, 3, 4, 8)]
        + plane_partners(x, y)
        + [dict(c=other)]
    )

    def piece(ref, m, core, chip):
        if m < 2:
            return ref.at[pl.ds(pl.multiple_of(512 * core + 32 * chip, 32), 32)]
        row = pl.multiple_of(192 * core + 48 * (chip // 4), 16)
        col = pl.multiple_of(256 * lax.rem(chip, 4), 128)
        return ref.at[pl.ds(row, 48), pl.ds(col, 256)]

    far = wrap(z + 8, NZ)
    own, second = (wg, wu, wd), (w2g, w2u, w2d)
    to_far = [
        remote(piece(own[m], m, c, me), piece(second[m], m, c, me), wz_send.at[m], wz_recv.at[m], z=far)
        for m in range(3)
    ]
    for cp in to_far:
        cp.start()

    sent = []
    for i in ORDER:
        to = wrap(z + DIST[i], NZ)
        sent.append(remote(sgt.at[i], gts.at[i], gt_send.at[i], gt_recv.at[i], z=to))
        sent.append(remote(st.at[i], ptok.at[i], t_send.at[i], t_recv.at[i], z=to))
        sent.append(remote(sg.at[i], pgrad.at[i], g_send.at[i], g_recv.at[i], z=to))
        if i < NS:
            j = NP + i
            sent.append(remote(st.at[j], stok.at[i], t_send.at[j], t_recv.at[j], z=to))
            sent.append(remote(sg.at[j], sgrad.at[i], g_send.at[j], g_recv.at[j], z=to))
    for cp in sent:
        cp.start()
    kept = [
        pltpu.make_async_copy(sgt.at[HOME], gts.at[HOME], loc.at[0]),
        pltpu.make_async_copy(st.at[HOME], ptok.at[HOME], loc.at[1]),
        pltpu.make_async_copy(sg.at[HOME], pgrad.at[HOME], loc.at[2]),
        pltpu.make_async_copy(st.at[NP + HOME], stok.at[HOME], loc.at[3]),
        pltpu.make_async_copy(sg.at[NP + HOME], sgrad.at[HOME], loc.at[4]),
    ]
    for cp in kept:
        cp.start()

    for cp in to_far:
        cp.wait_recv()

    def plane_copy(m, k):
        to = wrap(me + k, NCHIP)
        return remote(
            piece(second[m], m, c, me), piece(second[m], m, c, me),
            wp_send.at[m, k], wp_recv.at[m, k], x=to // 4, y=lax.rem(to, 4),
        )

    def arrived(m, k):
        frm = wrap(me - k + NCHIP, NCHIP)
        return remote(
            piece(second[m], m, c, frm), piece(second[m], m, c, frm),
            wp_send.at[m, k], wp_recv.at[m, k], x=frm // 4, y=lax.rem(frm, 4),
        )

    @pl.loop(1, NCHIP)
    def _(k):
        for m in range(3):
            plane_copy(m, k).start()

    @pl.loop(1, NCHIP)
    def _(k):
        for m in range(3):
            arrived(m, k).wait_recv()

    def half(ref, m):
        n = 512 if m < 2 else 192
        return ref.at[pl.ds(pl.multiple_of(n * c, n), n)]

    to_core = [
        remote(half(second[m], m), half(second[m], m), wc_send.at[m], wc_recv.at[m], c=other)
        for m in range(3)
    ]
    for cp in to_core:
        cp.start()
    for cp in to_far:
        cp.wait_send()

    @pl.loop(1, NCHIP)
    def _(k):
        for m in range(3):
            plane_copy(m, k).wait_send()

    for cp in to_core:
        cp.wait_send()
    for m in range(3):
        n = 512 if m < 2 else 192
        theirs = second[m].at[pl.ds(pl.multiple_of(n * other, n), n)]
        remote(theirs, theirs, wc_send.at[m], wc_recv.at[m], c=other).wait_recv()
    for cp in sent:
        cp.wait()
    for cp in kept:
        cp.wait()


def dispatch(st, sg, sgt, wg, wu, wd):
    hbm = pl.BlockSpec(memory_space=pl.ANY)
    dma = pltpu.SemaphoreType.DMA
    rows = lambda n: jax.ShapeDtypeStruct((n, CAP, 1024), BF16)
    return pl.pallas_call(
        dispatch_kernel,
        out_shape=(
            rows(NP), rows(NS), rows(NP), rows(NS),
            jax.ShapeDtypeStruct((NP, 8, 128), F32),
            jax.ShapeDtypeStruct(wg.shape, BF16),
            jax.ShapeDtypeStruct(wu.shape, BF16),
            jax.ShapeDtypeStruct(wd.shape, BF16),
        ),
        in_specs=[hbm] * 6,
        out_specs=(hbm,) * 8,
        scratch_shapes=[
            dma((16,)), dma((16,)), dma((16,)), dma((16,)), dma((9,)), dma((9,)),
            dma((3,)), dma((3,)), dma((3, 16)), dma((3, 16)), dma((3,)), dma((3,)), dma((5,)),
        ],
        compiler_params=pltpu.CompilerParams(collective_id=0, has_side_effects=True),
        name="dispatch",
    )(st, sg, sgt, wg, wu, wd)


def tail_kernel(
    oh, prob, tok, rw, prow, srow, gg,
    gp0, gp1, gp2, gs0, gs1, gs2,
    out_tok, out_w, out_r,
    rows_in, gg_in, sib, s0, rb, zs_out, zs_in, part, r_sib, r_half, r_in, r_z, r_zin, vbuf,
    row_send, row_recv, gg_send, gg_recv, sib_send, sib_recv, rs_send, rs_recv, zs_sem,
    r1_sem, r2_send, r2_recv, r3_send, r3_recv, r4_send, r4_recv, r5_send, r5_recv, r6_sem,
):
    x, y, c, z = place()
    me = x * 4 + y
    other = 1 - c
    far = wrap(z + 8, NZ)
    greet(
        [dict(z=wrap(z + d, NZ)) for d in range(1, NZ)]
        + plane_partners(x, y)
        + [dict(c=other)]
    )
    parts = (gp0, gp1, gp2, gs0, gs1, gs2)

    sent = [
        remote(gg.at[i], gg_in.at[i], gg_send.at[i], gg_recv.at[i], z=wrap(z - DIST[i] + NZ, NZ))
        for i in ORDER
    ]
    for cp in sent:
        cp.start()
    to_sib = [
        remote(parts[m].at[:, other], sib.at[m], sib_send.at[m], sib_recv.at[m], c=other)
        for m in range(6)
    ]
    for cp in to_sib:
        cp.start()
    rows = []
    for i in ORDER:
        to = wrap(z - DIST[i] + NZ, NZ)
        rows.append(remote(prow.at[i], rows_in.at[i], row_send.at[i], row_recv.at[i], z=to))
        if i < NS:
            j = NP + i
            rows.append(remote(srow.at[i], rows_in.at[j], row_send.at[j], row_recv.at[j], z=to))
    for cp in rows:
        cp.start()
    gg_in[HOME] = gg[HOME]
    rows_in[HOME] = prow[HOME]
    rows_in[NP + HOME] = srow[HOME]

    for cp in sent:
        cp.wait_recv()
    lane = lax.broadcasted_iota(jnp.int32, (CAP, 128), 1)
    sub = lax.broadcasted_iota(jnp.int32, (CAP, 128), 0)
    for g in range(16):
        i, s = (g, 0) if g < NP else (g - NP, 1)
        row = gg_in[i, s : s + 1, :]
        col = jnp.sum(jnp.where(lane == sub, row, 0.0), axis=1, keepdims=True)
        expert = 8 * lax.rem(z + RELATIVE[g], NZ)
        vbuf[g * CAP : (g + 1) * CAP, :] = jnp.where(lane == expert, col, 0.0).astype(BF16)
    grads = lax.dot_general(oh[...], vbuf[...], (((0,), (0,)), ((), ())), preferred_element_type=F32)
    p = prob[...]
    logit_grad = (p * (grads - jnp.sum(p * grads, axis=1, keepdims=True))).astype(BF16)
    part[...] = lax.dot_general(
        tok[...], logit_grad, (((0,), (0,)), ((), ())), preferred_element_type=F32
    ).reshape(part.shape)
    r1 = remote(part.at[other], r_sib, r1_sem.at[0], r1_sem.at[1], c=other)
    r1.start()

    def chip(k):
        to = wrap(me + k, NCHIP)
        return to, dict(x=to // 4, y=lax.rem(to, 4))

    r1.wait()
    r_half[...] = part[c] + r_sib[...]
    r_in[me] = r_half[me]

    def r2(k):
        to, where = chip(k)
        return remote(r_half.at[to], r_in.at[me], r2_send.at[k], r2_recv.at[k], **where)

    def r2_from(k):
        frm = wrap(me - k + NCHIP, NCHIP)
        return remote(r_half.at[0], r_in.at[frm], r2_send.at[k], r2_recv.at[k], x=frm // 4, y=lax.rem(frm, 4))

    @pl.loop(1, NCHIP)
    def _(k):
        r2(k).start()

    for cp in to_sib:
        cp.wait_recv()

    def rs(k):
        to, where = chip(k)
        return remote(s0.at[to], rb.at[me], rs_send.at[k], rs_recv.at[k], **where)

    def rs_from(k):
        frm = wrap(me - k + NCHIP, NCHIP)
        return remote(s0.at[0], rb.at[frm], rs_send.at[k], rs_recv.at[k], x=frm // 4, y=lax.rem(frm, 4))

    @pl.loop(1, NCHIP)
    def _(k):
        to, _w = chip(k)
        for m in range(6):
            s0[to, m] = (parts[m][to, c].astype(F32) + sib[m, to].astype(F32)).astype(BF16)
        rs(k).start()

    for m in range(6):
        rb[me, m] = (parts[m][me, c].astype(F32) + sib[m, me].astype(F32)).astype(BF16)

    @pl.loop(1, NCHIP)
    def _(k):
        r2_from(k).wait_recv()

    r_z[...] = jnp.sum(r_in[...], axis=0)

    def r3(k):
        to = wrap(z + k, NZ)
        return remote(r_z.at[to], r_zin.at[z], r3_send.at[k], r3_recv.at[k], z=to)

    def r3_from(k):
        frm = wrap(z - k + NZ, NZ)
        return remote(r_z.at[0], r_zin.at[frm], r3_send.at[k], r3_recv.at[k], z=frm)

    @pl.loop(1, NZ)
    def _(k):
        r3(k).start()

    r_zin[z] = r_z[z]

    for cp in rows:
        cp.wait_recv()
    out_tok[...] = (
        lax.dot_general(
            oh[...], rows_in[...].reshape(512, 1024), (((0,), (0,)), ((), ())), preferred_element_type=F32
        )
        + lax.dot_general(logit_grad, rw[...], (((1,), (1,)), ((), ())), preferred_element_type=F32)
    ).astype(BF16)

    @pl.loop(1, NZ)
    def _(k):
        r3_from(k).wait_recv()

    out_r[c, me, z] = jnp.sum(r_zin[...], axis=0)

    def r4(k):
        to = wrap(z + k, NZ)
        return remote(out_r.at[c, me, z], out_r.at[c, me, z], r4_send.at[k], r4_recv.at[k], z=to)

    def r4_from(k):
        frm = wrap(z - k + NZ, NZ)
        return remote(out_r.at[c, me, frm], out_r.at[c, me, frm], r4_send.at[k], r4_recv.at[k], z=frm)

    @pl.loop(1, NZ)
    def _(k):
        r4(k).start()

    @pl.loop(1, NZ)
    def _(k):
        r4_from(k).wait_recv()

    def r5(k):
        _to, where = chip(k)
        return remote(out_r.at[c, me], out_r.at[c, me], r5_send.at[k], r5_recv.at[k], **where)

    def r5_from(k):
        frm = wrap(me - k + NCHIP, NCHIP)
        return remote(out_r.at[c, frm], out_r.at[c, frm], r5_send.at[k], r5_recv.at[k], x=frm // 4, y=lax.rem(frm, 4))

    @pl.loop(1, NCHIP)
    def _(k):
        r5(k).start()

    @pl.loop(1, NCHIP)
    def _(k):
        rs_from(k).wait_recv()

    for m in range(3):
        zs_out[m] = jnp.sum(rb[:, 3 + m].astype(F32), axis=0).astype(BF16)
    zs = remote(zs_out, zs_in, zs_sem.at[0], zs_sem.at[1], z=far)
    zs.start()
    for m in range(3):
        out_w[m] = jnp.sum(rb[:, m].astype(F32), axis=0)

    @pl.loop(1, NCHIP)
    def _(k):
        r5_from(k).wait_recv()

    r6 = remote(out_r.at[c], out_r.at[c], r6_sem.at[0], r6_sem.at[1], c=other)
    r6.start()
    zs.wait()
    out_w[...] += zs_in[...].astype(F32)
    r6.wait_send()
    remote(out_r.at[other], out_r.at[other], r6_sem.at[0], r6_sem.at[1], c=other).wait_recv()
    for cp in sent + to_sib + rows:
        cp.wait_send()

    @pl.loop(1, NCHIP)
    def _(k):
        rs(k).wait_send()
        r2(k).wait_send()
        r3(k).wait_send()
        r4(k).wait_send()
        r5(k).wait_send()


def tail(oh, prob, tok, rw, prow, srow, gg, parts):
    vmem = pl.BlockSpec(memory_space=pltpu.VMEM)
    dma = pltpu.SemaphoreType.DMA
    V = pltpu.VMEM
    return pl.pallas_call(
        tail_kernel,
        out_shape=(
            jax.ShapeDtypeStruct((256, 1024), BF16),
            jax.ShapeDtypeStruct((3, 32, 384), F32),
            jax.ShapeDtypeStruct((2, 16, 16, 2, 128), F32),
        ),
        in_specs=[vmem] * 13,
        out_specs=(vmem,) * 3,
        scratch_shapes=[
            V((16, CAP, 1024), BF16), V((NP, 8, 128), F32),
            V((6, 16, 32, 384), BF16), V((16, 6, 32, 384), BF16), V((16, 6, 32, 384), BF16),
            V((3, 32, 384), BF16), V((3, 32, 384), BF16),
            V((2, 16, 16, 2, 128), F32), V((16, 16, 2, 128), F32), V((16, 16, 2, 128), F32),
            V((16, 16, 2, 128), F32), V((16, 2, 128), F32), V((16, 2, 128), F32),
            V((512, 128), BF16),
            dma((16,)), dma((16,)), dma((9,)), dma((9,)), dma((6,)), dma((6,)),
            dma((16,)), dma((16,)), dma((2,)),
            dma((2,)), dma((16,)), dma((16,)), dma((16,)), dma((16,)), dma((16,)), dma((16,)),
            dma((16,)), dma((16,)), dma((2,)),
        ],
        compiler_params=pltpu.CompilerParams(
            collective_id=1, has_side_effects=True, vmem_limit_bytes=48 << 20
        ),
        name="tail",
    )(oh, prob, tok, rw, prow, srow, gg, *parts)


def dot(a, b, ca, cb, out=F32):
    return lax.dot_general(a, b, (((ca,), (cb,)), ((), ())), preferred_element_type=out)


def expert(rows, grads, gates, wg, wu, wd):
    pre_gate = dot(rows, wg, 1, 0)
    pre_up = dot(rows, wu, 1, 0)
    sigma = jax.nn.sigmoid(pre_gate)
    active = (pre_gate * sigma * pre_up).astype(BF16)
    produced = dot(active, wd, 1, 0)
    gate_grad = jnp.sum(grads.astype(F32) * produced, axis=1).astype(BF16)
    out_grad = (gates[:, None] * grads.astype(F32)).astype(BF16)
    act_grad = dot(out_grad, wd, 1, 1)
    up_grad = (act_grad * pre_gate * sigma).astype(BF16)
    gate_pre = (act_grad * pre_up * sigma * (1.0 + pre_gate * (1.0 - sigma))).astype(BF16)
    back = (dot(gate_pre, wg, 1, 1) + dot(up_grad, wu, 1, 1)).astype(BF16)
    parts = (
        dot(rows, gate_pre, 0, 0).astype(BF16).reshape(16, 2, 32, 384),
        dot(rows, up_grad, 0, 0).astype(BF16).reshape(16, 2, 32, 384),
        dot(active, out_grad, 0, 0).astype(BF16).reshape(16, 2, 32, 384),
    )
    return back.reshape(-1, CAP, 1024), gate_grad.astype(F32), parts


def tiles(values):
    own = values[: NP * CAP].reshape(NP, 1, CAP)
    second = jnp.pad(values[NP * CAP :].reshape(NS, 1, CAP), ((0, NP - NS), (0, 0), (0, 0)))
    return jnp.pad(jnp.concatenate([own, second], axis=1), ((0, 0), (0, 6), (0, 128 - CAP)))


def local(tokens, grad_out, expert_ids, router_weight, wg, wu, wd):
    z = lax.axis_index("expert")
    wg, wu, wd = wg[0], wu[0], wd[0]
    experts = 8 * ((jnp.array(RELATIVE, jnp.int32) + z) % NZ)
    ids = expert_ids.T
    served = jnp.any(ids[:, None, :] == experts[None, :, None], axis=0)
    t = lax.broadcasted_iota(jnp.int32, (256, 256), 0)
    u = lax.broadcasted_iota(jnp.int32, (256, 256), 1)
    rank = dot(served.astype(BF16), (t < u).astype(BF16), 1, 0)
    slot = jnp.where(served, rank, -1.0)
    oh = (slot[:, None, :] == lax.broadcasted_iota(jnp.int32, (1, CAP, 1), 1).astype(F32)).astype(BF16)
    oh = oh.reshape(512, 256)
    logits = dot(tokens, router_weight, 1, 0)
    every = lax.broadcasted_iota(jnp.int32, (1, 1, 128), 2)
    mask = jnp.any(expert_ids[:, :, None] == every, axis=1)
    raised = jnp.where(mask, jnp.exp(logits), 0.0)
    prob = raised / jnp.sum(raised, axis=1, keepdims=True)
    slot_probs = dot(oh, prob.astype(BF16), 1, 0)
    at = jnp.repeat(experts, CAP)[:, None] == every[0]
    gates = jnp.sum(jnp.where(at, slot_probs, 0.0), axis=1)
    st = dot(oh, tokens, 1, 0, BF16).reshape(16, CAP, 1024)
    sg = dot(oh, grad_out, 1, 0, BF16).reshape(16, CAP, 1024)
    ptok, stok, pgrad, sgrad, gts, w2g, w2u, w2d = dispatch(st, sg, tiles(gates), wg, wu, wd)
    flat = lambda a: a.reshape(-1, 1024)
    prow, pgg, pparts = expert(flat(ptok), flat(pgrad), gts[:, 0, :CAP].reshape(-1), wg, wu, wd)
    srow, sgg, sparts = expert(flat(stok), flat(sgrad), gts[:NS, 1, :CAP].reshape(-1), w2g, w2u, w2d)
    grad_tokens, grads, router = tail(
        oh, prob, tokens, router_weight, prow, srow, tiles(jnp.concatenate([pgg, sgg])), pparts + sparts
    )
    return (
        grad_tokens,
        grads[0][None],
        grads[1][None],
        grads[2].reshape(1, 12, 1024),
        router.reshape(1024, 128),
    )


def solution(mesh):
    finer = Mesh(mesh.devices.reshape(4, 4, 2, NZ), AX)
    dp = AX[:3]
    return jax.shard_map(
        local,
        mesh=finer,
        in_specs=(
            P(AX, None), P(AX, None), P(AX, None), P(),
            P("expert", None, None), P("expert", None, None), P("expert", None, None),
        ),
        out_specs=(
            P(AX, None), P("expert", dp, None), P("expert", dp, None), P("expert", dp, None), P(),
        ),
        check_vma=False,
    )
```

```python
import jax
import jax.numpy as jnp
from jax import lax
from jax.experimental import pallas as pl
from jax.experimental.pallas import tpu as pltpu
from jax.sharding import Mesh
from jax.sharding import PartitionSpec as P

AX = ("dp_0", "dp_1", "dp_2", "expert")
MESH = pl.DeviceIdType.MESH
F32, BF16 = jnp.float32, jnp.bfloat16

NZ = 16
NCHIP = 16
CAP = 32
DIST = (-3, -2, -1, 0, 1, 2, 3, 4, -4)
RELATIVE = tuple(d % NZ for d in DIST) + tuple((d + 8) % NZ for d in DIST[:7])
NP, NS = 9, 7
HOME = 3
ORDER = (7, 8, 0, 6, 1, 5, 2, 4)


def wrap(v, n):
    return lax.rem(v + n, n)


def at(where):
    return {AX["xycz".index(k)]: v for k, v in where.items()}


def remote(src, dst, send, recv, **where):
    return pltpu.make_async_remote_copy(
        src_ref=src, dst_ref=dst, send_sem=send, recv_sem=recv, device_id=at(where), device_id_type=MESH
    )


def dot(a, b, ca, cb):
    return lax.dot_general(a, b, (((ca,), (cb,)), ((), ())), preferred_element_type=F32)


def starts(copies):
    for cp in copies:
        cp.start()


def whole(
    tok_h, grad_h, ids_h, rw_h, wg_h, wu_h, wd_h,
    out_tok, out_w, out_d, out_r,
    tok, grad, ids, rw, w1, w1d, w2, w2d,
    oh, prob, st, sg, sgt, sel,
    ptok, stok, pgrad, sgrad, gts,
    pre, act, og, gu, ac, made,
    prow, srow, gg, rows_in, gg_in, vbuf,
    pa, pd, sa, sd, sib_pa, sib_pd, sib_sa, sib_sd,
    s_pa, s_pd, s_sa, s_sd, rb_pa, rb_pd, rb_sa, rb_sd,
    za_out, zd_out, za_in, zd_in,
    part, r_sib, r_half, r_in, r_z, r_zin,
    loc, t_send, t_recv, g_send, g_recv, gt_send, gt_recv,
    wz_send, wz_recv, wp_send, wp_recv, wc_send, wc_recv,
    row_send, row_recv, gg_send, gg_recv,
    sib_send, sib_recv, rs_send, rs_recv, zs_sem,
    r1_sem, r2_send, r2_recv, r3_send, r3_recv, r4_send, r4_recv, r5_send, r5_recv, r6_sem,
):
    x, y, c, z = tuple(lax.axis_index(a) for a in AX)
    me = x * 4 + y
    other = 1 - c
    far = wrap(z + 8, NZ)

    fetch = [
        pltpu.make_async_copy(ids_h, ids, loc.at[0]),
        pltpu.make_async_copy(tok_h, tok, loc.at[1]),
        pltpu.make_async_copy(rw_h, rw, loc.at[2]),
        pltpu.make_async_copy(grad_h, grad, loc.at[3]),
        pltpu.make_async_copy(wg_h, w1.at[:, pl.ds(0, 384)], loc.at[4]),
        pltpu.make_async_copy(wu_h, w1.at[:, pl.ds(384, 384)], loc.at[5]),
        pltpu.make_async_copy(wd_h, w1d, loc.at[6]),
    ]
    starts(fetch)

    barrier = pltpu.get_barrier_semaphore()
    partners = [dict(z=wrap(z + d, NZ)) for d in range(1, NZ)] + [dict(c=other)]
    partners += [
        dict(x=wrap(x + dx, 4), y=wrap(y + dy, 4)) for dx in range(4) for dy in range(4) if dx or dy
    ]
    for where in partners:
        pl.semaphore_signal(barrier, inc=1, device_id=at(where), device_id_type=MESH)

    def chip(k):
        to = wrap(me + k, NCHIP)
        return to, dict(x=to // 4, y=lax.rem(to, 4))

    def chip_from(k):
        frm = wrap(me - k + NCHIP, NCHIP)
        return frm, dict(x=frm // 4, y=lax.rem(frm, 4))

    lane = lax.broadcasted_iota(jnp.int32, (CAP, 128), 1)
    sub = lax.broadcasted_iota(jnp.int32, (CAP, 128), 0)

    def expert_of(g):
        return 8 * lax.rem(z + RELATIVE[g], NZ)

    def to_row(col):
        return jnp.sum(jnp.where(lane == sub, col, 0.0), axis=0, keepdims=True)

    def to_col(row):
        return jnp.sum(jnp.where(lane == sub, row, 0.0), axis=1, keepdims=True)

    fetch[0].wait()
    every = lax.broadcasted_iota(jnp.int32, (256, 128), 1)
    named = ids[:, 0:1] == every
    for k in range(1, 8):
        named = jnp.logical_or(named, ids[:, k : k + 1] == every)
    mask = jnp.where(named, 1.0, 0.0).astype(BF16)
    row16 = lax.broadcasted_iota(jnp.int32, (16, 128), 0)
    rel = jnp.zeros((16, 128), jnp.int32)
    for g in range(16):
        rel = jnp.where(row16 == g, expert_of(g), rel)
    mine = jnp.where(lax.broadcasted_iota(jnp.int32, (16, 128), 1) == rel, 1.0, 0.0).astype(BF16)
    served = dot(mine, mask, 1, 1)
    before = lax.broadcasted_iota(jnp.int32, (256, 256), 0) < lax.broadcasted_iota(jnp.int32, (256, 256), 1)
    rank = dot(served.astype(BF16), jnp.where(before, 1.0, 0.0).astype(BF16), 1, 0)
    slot = jnp.where(served > 0.5, rank, -1.0)
    want = lax.broadcasted_iota(jnp.int32, (CAP, 256), 0).astype(F32)
    for g in range(16):
        oh[g * CAP : (g + 1) * CAP, :] = jnp.where(slot[g : g + 1, :] == want, 1.0, 0.0).astype(BF16)
    fetch[1].wait()
    st[...] = dot(oh[...], tok[...], 1, 0).astype(BF16).reshape(st.shape)
    fetch[2].wait()
    logits = dot(tok[...], rw[...], 1, 0)
    raised = jnp.where(named, jnp.exp(logits), 0.0)
    prob[...] = raised / jnp.sum(raised, axis=1, keepdims=True)
    slot_prob = dot(oh[...], prob[...].astype(BF16), 1, 0)
    sgt[...] = jnp.zeros_like(sgt)
    for g in range(16):
        i, s = (g, 0) if g < NP else (g - NP, 1)
        col = jnp.sum(
            jnp.where(lane == expert_of(g), slot_prob[g * CAP : (g + 1) * CAP, :], 0.0), axis=1, keepdims=True
        )
        sgt[i, s : s + 1, :] = to_row(col)
    fetch[3].wait()
    sg[...] = dot(oh[...], grad[...], 1, 0).astype(BF16).reshape(sg.shape)
    for cp in fetch[4:]:
        cp.wait()

    pl.semaphore_wait(barrier, len(partners))

    def piece(ref, m, core, p):
        if m == 0:
            return ref.at[pl.ds(pl.multiple_of(512 * core + 32 * p, 32), 32)]
        row = pl.multiple_of(192 * core + 48 * (p // 4), 16)
        col = pl.multiple_of(256 * lax.rem(p, 4), 128)
        return ref.at[pl.ds(row, 48), pl.ds(col, 256)]

    own, second = (w1, w1d), (w2, w2d)
    to_far = [
        remote(piece(own[m], m, c, me), piece(second[m], m, c, me), wz_send.at[m], wz_recv.at[m], z=far)
        for m in range(2)
    ]
    starts(to_far)

    first, later = [], []
    for i in ORDER:
        to = wrap(z + DIST[i], NZ)
        first.append(remote(sgt.at[i], gts.at[i], gt_send.at[i], gt_recv.at[i], z=to))
        first.append(remote(st.at[i], ptok.at[i], t_send.at[i], t_recv.at[i], z=to))
        first.append(remote(sg.at[i], pgrad.at[i], g_send.at[i], g_recv.at[i], z=to))
        if i < NS:
            j = NP + i
            later.append(remote(st.at[j], stok.at[i], t_send.at[j], t_recv.at[j], z=to))
            later.append(remote(sg.at[j], sgrad.at[i], g_send.at[j], g_recv.at[j], z=to))
    starts(first)
    starts(later)
    gts[HOME] = sgt[HOME]
    ptok[HOME] = st[HOME]
    pgrad[HOME] = sg[HOME]
    stok[HOME] = st[NP + HOME]
    sgrad[HOME] = sg[NP + HOME]

    q = lax.broadcasted_iota(jnp.int32, (384, 512), 1)
    unit = lax.broadcasted_iota(jnp.int32, (384, 512), 0)
    block, k16 = q // 16, lax.rem(q, 16)
    sel[...] = jnp.where(jnp.logical_and(unit == block * 12 + k16, k16 < 12), 1.0, 0.0).astype(BF16)

    for cp in to_far:
        cp.wait_recv()

    def plane_copy(m, k):
        _to, where = chip(k)
        mine_ = piece(second[m], m, c, me)
        return remote(mine_, mine_, wp_send.at[m, k], wp_recv.at[m, k], **where)

    def plane_from(m, k):
        frm, where = chip_from(k)
        theirs = piece(second[m], m, c, frm)
        return remote(theirs, theirs, wp_send.at[m, k], wp_recv.at[m, k], **where)

    @pl.loop(1, NCHIP)
    def _(k):
        for m in range(2):
            plane_copy(m, k).start()

    @pl.loop(1, NCHIP)
    def _(k):
        for m in range(2):
            plane_from(m, k).wait_recv()

    def half(m, core):
        n = 512 if m == 0 else 192
        ref = second[m].at[pl.ds(pl.multiple_of(n * core, n), n)]
        return remote(ref, ref, wc_send.at[m], wc_recv.at[m], c=other)

    for m in range(2):
        half(m, c).start()

    def expert_rows(n, rows, grads, s, w, wd):
        m = n * CAP

        @pl.loop(0, n)
        def _(g):
            og[g] = (to_col(gts[g, s : s + 1, :]) * grads[g].astype(F32)).astype(BF16)

        pre[0:n] = dot(rows[...].reshape(m, 1024), w[...], 1, 0).reshape(n, CAP, 768)
        act[0:n] = dot(og[0:n].reshape(m, 1024), wd[...], 1, 1).reshape(n, CAP, 384)

        @pl.loop(0, n)
        def _(g):
            pg, pu, ag = pre[g, :, 0:384], pre[g, :, 384:768], act[g]
            sigma = lax.logistic(pg)
            ac[g] = (pg * sigma * pu).astype(BF16)
            gu[g, :, 0:384] = (ag * pu * sigma * (1.0 + pg * (1.0 - sigma))).astype(BF16)
            gu[g, :, 384:768] = (ag * pg * sigma).astype(BF16)

    def expert_parts(n, rows, a, d):
        m = n * CAP
        a[...] = dot(rows[...].reshape(m, 1024), gu[0:n].reshape(m, 768), 0, 0).astype(BF16).reshape(a.shape)
        spread = dot(ac[0:n].reshape(m, 384), sel[...], 1, 0).astype(BF16)
        d[...] = dot(spread, og[0:n].reshape(m, 1024), 0, 0).astype(BF16).reshape(d.shape)

    def expert_gates(n, grads, s, wd):
        m = n * CAP
        made[0:n] = dot(ac[0:n].reshape(m, 384), wd[...], 1, 0).reshape(n, CAP, 1024)

        @pl.loop(0, n)
        def _(g):
            col = jnp.sum(grads[g].astype(F32) * made[g], axis=1, keepdims=True)
            gg[g, s] = to_row(col.astype(BF16).astype(F32))

    def expert_back(n, w, back):
        m = n * CAP
        back[...] = dot(gu[0:n].reshape(m, 768), w[...], 1, 1).astype(BF16).reshape(back.shape)

    def give_gates(s, n):
        return [
            remote(gg.at[i, s], gg_in.at[i, s], gg_send.at[s, i], gg_recv.at[s, i], z=wrap(z - DIST[i] + NZ, NZ))
            for i in ORDER
            if i < n
        ]

    def give_rows(back, n, base):
        return [
            remote(back.at[i], rows_in.at[base + i], row_send.at[base + i], row_recv.at[base + i], z=wrap(z - DIST[i] + NZ, NZ))
            for i in ORDER
            if i < n
        ]

    def swap_core(a, d, a_in, d_in, e):
        return [
            remote(a.at[:, other], a_in, sib_send.at[e, 0], sib_recv.at[e, 0], c=other),
            remote(d.at[:, other], d_in, sib_send.at[e, 1], sib_recv.at[e, 1], c=other),
        ]

    def add_core(a, d, a_in, d_in, s_a, s_d):
        @pl.loop(0, NCHIP)
        def _(k):
            s_a[k] = (a[k, c].astype(F32) + a_in[k].astype(F32)).astype(BF16)
            s_d[k] = (d[k, c].astype(F32) + d_in[k].astype(F32)).astype(BF16)

    def scatter(e, k, s_a, s_d, rb_a, rb_d):
        to, where = chip(k)
        return [
            remote(s_a.at[to], rb_a.at[me], rs_send.at[e, 0, k], rs_recv.at[e, 0, k], **where),
            remote(s_d.at[to], rb_d.at[me], rs_send.at[e, 1, k], rs_recv.at[e, 1, k], **where),
        ]

    def scattered(e, k, s_a, s_d, rb_a, rb_d):
        frm, where = chip_from(k)
        return [
            remote(s_a.at[0], rb_a.at[frm], rs_send.at[e, 0, k], rs_recv.at[e, 0, k], **where),
            remote(s_d.at[0], rb_d.at[frm], rs_send.at[e, 1, k], rs_recv.at[e, 1, k], **where),
        ]

    for cp in first:
        cp.wait_recv()
    expert_rows(NP, ptok, pgrad, 0, w1, w1d)
    expert_parts(NP, ptok, pa, pd)
    swap_p = swap_core(pa, pd, sib_pa, sib_pd, 0)
    starts(swap_p)
    expert_gates(NP, pgrad, 0, w1d)
    gates_p = give_gates(0, NP)
    starts(gates_p)
    expert_back(NP, w1, prow)
    rows_p = give_rows(prow, NP, 0)
    starts(rows_p)
    rows_in[HOME] = prow[HOME]
    gg_in[HOME, 0] = gg[HOME, 0]
    for cp in swap_p:
        cp.wait_recv()
    add_core(pa, pd, sib_pa, sib_pd, s_pa, s_pd)
    arrays_p = (s_pa, s_pd, rb_pa, rb_pd)

    @pl.loop(1, NCHIP)
    def _(k):
        starts(scatter(0, k, *arrays_p))

    rb_pa[me] = s_pa[me]
    rb_pd[me] = s_pd[me]

    for m in range(2):
        half(m, other).wait_recv()
    for cp in later:
        cp.wait_recv()
    expert_rows(NS, stok, sgrad, 1, w2, w2d)
    expert_gates(NS, sgrad, 1, w2d)
    gates_s = give_gates(1, NS)
    starts(gates_s)
    expert_parts(NS, stok, sa, sd)
    swap_s = swap_core(sa, sd, sib_sa, sib_sd, 1)
    starts(swap_s)
    expert_back(NS, w2, srow)
    rows_s = give_rows(srow, NS, NP)
    starts(rows_s)
    rows_in[NP + HOME] = srow[HOME]
    gg_in[HOME, 1] = gg[HOME, 1]

    for cp in gates_p + gates_s:
        cp.wait_recv()
    for g in range(16):
        i, s = (g, 0) if g < NP else (g - NP, 1)
        col = to_col(gg_in[i, s])
        vbuf[g * CAP : (g + 1) * CAP, :] = jnp.where(lane == expert_of(g), col, 0.0).astype(BF16)
    grads = dot(oh[...], vbuf[...], 0, 0)
    p = prob[...]
    logit_grad = (p * (grads - jnp.sum(p * grads, axis=1, keepdims=True))).astype(BF16)
    part[...] = dot(tok[...], logit_grad, 0, 0).reshape(part.shape)
    r1 = remote(part.at[other], r_sib, r1_sem.at[0], r1_sem.at[1], c=other)
    r1.start()
    for cp in swap_s:
        cp.wait_recv()
    add_core(sa, sd, sib_sa, sib_sd, s_sa, s_sd)
    arrays_s = (s_sa, s_sd, rb_sa, rb_sd)
    r1.wait()
    r_half[...] = part[c] + r_sib[...]
    r_in[me] = r_half[me]

    def r2(k):
        to, where = chip(k)
        return remote(r_half.at[to], r_in.at[me], r2_send.at[k], r2_recv.at[k], **where)

    def r2_from(k):
        frm, where = chip_from(k)
        return remote(r_half.at[0], r_in.at[frm], r2_send.at[k], r2_recv.at[k], **where)

    @pl.loop(1, NCHIP)
    def _(k):
        r2(k).start()

    @pl.loop(1, NCHIP)
    def _(k):
        starts(scatter(1, k, *arrays_s))

    rb_sa[me] = s_sa[me]
    rb_sd[me] = s_sd[me]

    @pl.loop(1, NCHIP)
    def _(k):
        r2_from(k).wait_recv()

    r_z[...] = jnp.sum(r_in[...], axis=0)

    def r3(k):
        return remote(r_z.at[wrap(z + k, NZ)], r_zin.at[z], r3_send.at[k], r3_recv.at[k], z=wrap(z + k, NZ))

    def r3_from(k):
        frm = wrap(z - k + NZ, NZ)
        return remote(r_z.at[0], r_zin.at[frm], r3_send.at[k], r3_recv.at[k], z=frm)

    @pl.loop(1, NZ)
    def _(k):
        r3(k).start()

    r_zin[z] = r_z[z]

    for cp in rows_p + rows_s:
        cp.wait_recv()
    out_tok[...] = (
        dot(oh[...], rows_in[...].reshape(512, 1024), 0, 0) + dot(logit_grad, rw[...], 1, 1)
    ).astype(BF16)

    @pl.loop(1, NZ)
    def _(k):
        r3_from(k).wait_recv()

    out_r[c, me, z] = jnp.sum(r_zin[...], axis=0)

    def r4(k):
        ref = out_r.at[c, me, z]
        return remote(ref, ref, r4_send.at[k], r4_recv.at[k], z=wrap(z + k, NZ))

    def r4_from(k):
        frm = wrap(z - k + NZ, NZ)
        ref = out_r.at[c, me, frm]
        return remote(ref, ref, r4_send.at[k], r4_recv.at[k], z=frm)

    @pl.loop(1, NZ)
    def _(k):
        r4(k).start()

    @pl.loop(1, NCHIP)
    def _(k):
        for cp in scattered(0, k, *arrays_p):
            cp.wait_recv()

    out_w[...] = jnp.sum(rb_pa[...].astype(F32), axis=0)
    out_d[...] = jnp.sum(rb_pd[...].astype(F32), axis=0)

    @pl.loop(1, NZ)
    def _(k):
        r4_from(k).wait_recv()

    def r5(k):
        _to, where = chip(k)
        ref = out_r.at[c, me]
        return remote(ref, ref, r5_send.at[k], r5_recv.at[k], **where)

    def r5_from(k):
        frm, where = chip_from(k)
        ref = out_r.at[c, frm]
        return remote(ref, ref, r5_send.at[k], r5_recv.at[k], **where)

    @pl.loop(1, NCHIP)
    def _(k):
        r5(k).start()

    @pl.loop(1, NCHIP)
    def _(k):
        for cp in scattered(1, k, *arrays_s):
            cp.wait_recv()

    za_out[...] = jnp.sum(rb_sa[...].astype(F32), axis=0).astype(BF16)
    zd_out[...] = jnp.sum(rb_sd[...].astype(F32), axis=0).astype(BF16)
    zs = [
        remote(za_out, za_in, zs_sem.at[0], zs_sem.at[1], z=far),
        remote(zd_out, zd_in, zs_sem.at[2], zs_sem.at[3], z=far),
    ]
    starts(zs)

    @pl.loop(1, NCHIP)
    def _(k):
        r5_from(k).wait_recv()

    r6 = remote(out_r.at[c], out_r.at[c], r6_sem.at[0], r6_sem.at[1], c=other)
    r6.start()
    for cp in to_far + first + later + swap_p + swap_s + gates_p + gates_s + rows_p + rows_s:
        cp.wait_send()
    for m in range(2):
        half(m, c).wait_send()

    @pl.loop(1, NCHIP)
    def _(k):
        for m in range(2):
            plane_copy(m, k).wait_send()
        for cp in scatter(0, k, *arrays_p) + scatter(1, k, *arrays_s):
            cp.wait_send()
        for r in (r2, r3, r4, r5):
            r(k).wait_send()

    for cp in zs:
        cp.wait()
    out_w[...] += za_in[...].astype(F32)
    out_d[...] += zd_in[...].astype(F32)
    r6.wait_send()
    remote(out_r.at[other], out_r.at[other], r6_sem.at[0], r6_sem.at[1], c=other).wait_recv()


def local(tokens, grad_out, expert_ids, router_weight, wg, wu, wd):
    hbm = pl.BlockSpec(memory_space=pl.ANY)
    vmem = pl.BlockSpec(memory_space=pltpu.VMEM)
    dma = pltpu.SemaphoreType.DMA
    V = pltpu.VMEM
    blocks = [V((NCHIP, 32, 768), BF16), V((NCHIP, 16, 1024), BF16)]
    grad_tokens, grads, down, router = pl.pallas_call(
        whole,
        out_shape=(
            jax.ShapeDtypeStruct((256, 1024), BF16),
            jax.ShapeDtypeStruct((32, 768), F32),
            jax.ShapeDtypeStruct((16, 1024), F32),
            jax.ShapeDtypeStruct((2, 16, 16, 2, 128), F32),
        ),
        in_specs=[hbm] * 7,
        out_specs=(vmem,) * 4,
        scratch_shapes=[
            V((256, 1024), BF16), V((256, 1024), BF16), V((256, 8), jnp.int32), V((1024, 128), BF16),
            V((1024, 768), BF16), V((384, 1024), BF16), V((1024, 768), BF16), V((384, 1024), BF16),
            V((512, 256), BF16), V((256, 128), F32), V((16, CAP, 1024), BF16), V((16, CAP, 1024), BF16),
            V((NP, 8, 128), F32), V((384, 512), BF16),
            V((NP, CAP, 1024), BF16), V((NS, CAP, 1024), BF16), V((NP, CAP, 1024), BF16), V((NS, CAP, 1024), BF16),
            V((NP, 8, 128), F32),
            V((NP, CAP, 768), F32), V((NP, CAP, 384), F32), V((NP, CAP, 1024), BF16),
            V((NP, CAP, 768), BF16), V((NP, CAP, 384), BF16), V((NP, CAP, 1024), F32),
            V((NP, CAP, 1024), BF16), V((NS, CAP, 1024), BF16), V((NP, 2, 1, 128), F32),
            V((16, CAP, 1024), BF16), V((NP, 2, 1, 128), F32), V((512, 128), BF16),
            V((16, 2, 32, 768), BF16), V((16, 2, 16, 1024), BF16),
            V((16, 2, 32, 768), BF16), V((16, 2, 16, 1024), BF16),
            *blocks, *blocks, *blocks, *blocks, *blocks, *blocks,
            V((32, 768), BF16), V((16, 1024), BF16), V((32, 768), BF16), V((16, 1024), BF16),
            V((2, 16, 16, 2, 128), F32), V((16, 16, 2, 128), F32), V((16, 16, 2, 128), F32),
            V((16, 16, 2, 128), F32), V((16, 2, 128), F32), V((16, 2, 128), F32),
            dma((7,)), dma((16,)), dma((16,)), dma((16,)), dma((16,)), dma((9,)), dma((9,)),
            dma((2,)), dma((2,)), dma((2, 16)), dma((2, 16)), dma((2,)), dma((2,)),
            dma((16,)), dma((16,)), dma((2, 9)), dma((2, 9)),
            dma((2, 2)), dma((2, 2)), dma((2, 2, 16)), dma((2, 2, 16)), dma((4,)),
            dma((2,)), dma((16,)), dma((16,)), dma((16,)), dma((16,)), dma((16,)), dma((16,)),
            dma((16,)), dma((16,)), dma((2,)),
        ],
        compiler_params=pltpu.CompilerParams(
            collective_id=0, has_side_effects=True, vmem_limit_bytes=58 << 20
        ),
        name="whole",
    )(tokens, grad_out, expert_ids, router_weight, wg[0], wu[0], wd[0])
    return (
        grad_tokens,
        grads[None, :, :384],
        grads[None, :, 384:],
        down[None, :12],
        router.reshape(1024, 128),
    )


def solution(mesh):
    finer = Mesh(mesh.devices.reshape(4, 4, 2, NZ), AX)
    dp = AX[:3]
    return jax.shard_map(
        local,
        mesh=finer,
        in_specs=(
            P(AX, None), P(AX, None), P(AX, None), P(),
            P("expert", None, None), P("expert", None, None), P("expert", None, None),
        ),
        out_specs=(
            P(AX, None), P("expert", dp, None), P("expert", dp, None), P("expert", dp, None), P(),
        ),
        check_vma=False,
    )
```

```python
import jax
import jax.numpy as jnp
from jax import lax
from jax.experimental import pallas as pl
from jax.experimental.pallas import tpu as pltpu
from jax.sharding import Mesh
from jax.sharding import PartitionSpec as P

AX = ("dp_0", "dp_1", "dp_2", "expert")
MESH = pl.DeviceIdType.MESH
F32, BF16 = jnp.float32, jnp.bfloat16

NZ = 16
NCHIP = 16
CAP = 32
DIST = (-3, -2, -1, 0, 1, 2, 3, 4, -4)
RELATIVE = tuple(d % NZ for d in DIST) + tuple((d + 8) % NZ for d in DIST[:7])
NP, NS = 9, 7
HOME = 3
ORDER = (7, 8, 0, 6, 1, 5, 2, 4)
NDP = 32


def wrap(v, n):
    return lax.rem(v + n, n)


def at(where):
    return {AX["xycz".index(k)]: v for k, v in where.items()}


def remote(src, dst, send, recv, **where):
    return pltpu.make_async_remote_copy(
        src_ref=src, dst_ref=dst, send_sem=send, recv_sem=recv, device_id=at(where), device_id_type=MESH
    )


def dot(a, b, ca, cb):
    return lax.dot_general(a, b, (((ca,), (cb,)), ((), ())), preferred_element_type=F32)


def starts(copies):
    for cp in copies:
        cp.start()


def whole(
    tok_h, grad_h, ids_h, rw_h, wg_h, wu_h, wd_h,
    out_tok, out_g, out_u, out_d, out_r,
    tok, grad, ids, rw, w1, w1d, w2, w2d,
    oh, prob, st, sg, sgt, sel,
    ptok, stok, pgrad, sgrad, gts,
    pre, act, og, gu, ac, made,
    prow, srow, gg, rows_in, gg_in, vbuf,
    pa, pd, sa, sd, sib_pa, sib_pd, sib_sa, sib_sd,
    s_pa, s_pd, s_sa, s_sd, rb_pa, rb_pd, rb_sa, rb_sd,
    za_out, zd_out, za_in, zd_in,
    total_d, part, r_in, r_zin, r_out,
    loc, t_send, t_recv, g_send, g_recv, gt_send, gt_recv,
    wz_send, wz_recv, wp_send, wp_recv, wc_send, wc_recv,
    row_send, row_recv, gg_send, gg_recv,
    sib_send, sib_recv, rs_send, rs_recv, zs_sem,
    r2_send, r2_recv, r3_send, r3_recv, r5_send, r5_recv,
):
    x, y, c, z = tuple(lax.axis_index(a) for a in AX)
    me = x * 4 + y
    other = 1 - c
    far = wrap(z + 8, NZ)

    fetch = [
        pltpu.make_async_copy(ids_h, ids, loc.at[0]),
        pltpu.make_async_copy(tok_h, tok, loc.at[1]),
        pltpu.make_async_copy(rw_h, rw, loc.at[2]),
        pltpu.make_async_copy(grad_h, grad, loc.at[3]),
        pltpu.make_async_copy(wg_h, w1.at[:, pl.ds(0, 384)], loc.at[4]),
        pltpu.make_async_copy(wu_h, w1.at[:, pl.ds(384, 384)], loc.at[5]),
        pltpu.make_async_copy(wd_h, w1d, loc.at[6]),
    ]
    starts(fetch)

    barrier = pltpu.get_barrier_semaphore()
    mine32 = me * 2 + c

    def plane(k):
        to = wrap(mine32 + k, NDP)
        return to, dict(x=to // 8, y=lax.rem(to // 2, 4), c=lax.rem(to, 2))

    def plane_back(k):
        frm = wrap(mine32 - k + NDP, NDP)
        return frm, dict(x=frm // 8, y=lax.rem(frm // 2, 4), c=lax.rem(frm, 2))

    partners = [dict(z=wrap(z + d, NZ)) for d in range(1, NZ)] + [plane(k)[1] for k in range(1, NDP)]
    for where in partners:
        pl.semaphore_signal(barrier, inc=1, device_id=at(where), device_id_type=MESH)

    def chip(k):
        to = wrap(me + k, NCHIP)
        return to, dict(x=to // 4, y=lax.rem(to, 4))

    def chip_from(k):
        frm = wrap(me - k + NCHIP, NCHIP)
        return frm, dict(x=frm // 4, y=lax.rem(frm, 4))

    lane = lax.broadcasted_iota(jnp.int32, (CAP, 128), 1)
    sub = lax.broadcasted_iota(jnp.int32, (CAP, 128), 0)

    def expert_of(g):
        return 8 * lax.rem(z + RELATIVE[g], NZ)

    def to_row(col):
        return jnp.sum(jnp.where(lane == sub, col, 0.0), axis=0, keepdims=True)

    def to_col(row):
        return jnp.sum(jnp.where(lane == sub, row, 0.0), axis=1, keepdims=True)

    fetch[0].wait()
    every = lax.broadcasted_iota(jnp.int32, (128, 256), 0)
    names = ids[0:1, :] == every
    for k in range(1, 8):
        names = jnp.logical_or(names, ids[k : k + 1, :] == every)
    mask = jnp.where(names, 1.0, 0.0).astype(BF16)
    unit = lax.broadcasted_iota(jnp.int32, (128, 128), 0) == lax.broadcasted_iota(jnp.int32, (128, 128), 1)
    named = dot(mask, jnp.where(unit, 1.0, 0.0).astype(BF16), 0, 0) > 0.5
    row16 = lax.broadcasted_iota(jnp.int32, (16, 128), 0)
    rel = jnp.zeros((16, 128), jnp.int32)
    for g in range(16):
        rel = jnp.where(row16 == g, expert_of(g), rel)
    mine = jnp.where(lax.broadcasted_iota(jnp.int32, (16, 128), 1) == rel, 1.0, 0.0).astype(BF16)
    served = dot(mine, mask, 1, 0)
    before = lax.broadcasted_iota(jnp.int32, (256, 256), 0) < lax.broadcasted_iota(jnp.int32, (256, 256), 1)
    rank = dot(served.astype(BF16), jnp.where(before, 1.0, 0.0).astype(BF16), 1, 0)
    slot = jnp.where(served > 0.5, rank, -1.0)
    want = lax.broadcasted_iota(jnp.int32, (CAP, 256), 0).astype(F32)
    for g in range(16):
        oh[g * CAP : (g + 1) * CAP, :] = jnp.where(slot[g : g + 1, :] == want, 1.0, 0.0).astype(BF16)
    fetch[1].wait()
    st[...] = dot(oh[...], tok[...], 1, 0).astype(BF16).reshape(st.shape)
    fetch[2].wait()
    logits = dot(tok[...], rw[...], 1, 0)
    raised = jnp.where(named, jnp.exp(logits), 0.0)
    prob[...] = raised / jnp.sum(raised, axis=1, keepdims=True)
    slot_prob = dot(oh[...], prob[...].astype(BF16), 1, 0)
    sgt[...] = jnp.zeros_like(sgt)
    for g in range(16):
        i, s = (g, 0) if g < NP else (g - NP, 1)
        col = jnp.sum(
            jnp.where(lane == expert_of(g), slot_prob[g * CAP : (g + 1) * CAP, :], 0.0), axis=1, keepdims=True
        )
        sgt[i, s : s + 1, :] = to_row(col)
    fetch[3].wait()
    sg[...] = dot(oh[...], grad[...], 1, 0).astype(BF16).reshape(sg.shape)
    for cp in fetch[4:]:
        cp.wait()

    pl.semaphore_wait(barrier, len(partners))

    def piece(ref, m, core, p):
        if m == 0:
            return ref.at[pl.ds(pl.multiple_of(512 * core + 32 * p, 32), 32)]
        row = pl.multiple_of(192 * core + 48 * (p // 4), 16)
        col = pl.multiple_of(256 * lax.rem(p, 4), 128)
        return ref.at[pl.ds(row, 48), pl.ds(col, 256)]

    own, second = (w1, w1d), (w2, w2d)
    to_far = [
        remote(piece(own[m], m, c, me), piece(second[m], m, c, me), wz_send.at[m], wz_recv.at[m], z=far)
        for m in range(2)
    ]
    starts(to_far)

    first, later = [], []
    for i in ORDER:
        to = wrap(z + DIST[i], NZ)
        first.append(remote(sgt.at[i], gts.at[i], gt_send.at[i], gt_recv.at[i], z=to))
        later.append(remote(st.at[i], ptok.at[i], t_send.at[i], t_recv.at[i], z=to))
        later.append(remote(sg.at[i], pgrad.at[i], g_send.at[i], g_recv.at[i], z=to))
        if i < NS:
            j = NP + i
            first.append(remote(st.at[j], stok.at[i], t_send.at[j], t_recv.at[j], z=to))
            first.append(remote(sg.at[j], sgrad.at[i], g_send.at[j], g_recv.at[j], z=to))
    starts(first)
    starts(later)
    gts[HOME] = sgt[HOME]
    ptok[HOME] = st[HOME]
    pgrad[HOME] = sg[HOME]
    stok[HOME] = st[NP + HOME]
    sgrad[HOME] = sg[NP + HOME]

    q = lax.broadcasted_iota(jnp.int32, (384, 512), 1)
    unit = lax.broadcasted_iota(jnp.int32, (384, 512), 0)
    block, k16 = q // 16, lax.rem(q, 16)
    sel[...] = jnp.where(jnp.logical_and(unit == block * 12 + k16, k16 < 12), 1.0, 0.0).astype(BF16)

    for cp in to_far:
        cp.wait_recv()

    def plane_copy(m, k):
        _to, where = chip(k)
        mine_ = piece(second[m], m, c, me)
        return remote(mine_, mine_, wp_send.at[m, k], wp_recv.at[m, k], **where)

    def plane_from(m, k):
        frm, where = chip_from(k)
        theirs = piece(second[m], m, c, frm)
        return remote(theirs, theirs, wp_send.at[m, k], wp_recv.at[m, k], **where)

    @pl.loop(1, NCHIP)
    def _(k):
        for m in range(2):
            plane_copy(m, k).start()

    @pl.loop(1, NCHIP)
    def _(k):
        for m in range(2):
            plane_from(m, k).wait_recv()

    def half(m, core):
        n = 512 if m == 0 else 192
        ref = second[m].at[pl.ds(pl.multiple_of(n * core, n), n)]
        return remote(ref, ref, wc_send.at[m], wc_recv.at[m], c=other)

    for m in range(2):
        half(m, c).start()

    def expert_rows(n, rows, grads, s, w, wd):
        m = n * CAP

        @pl.loop(0, n)
        def _(g):
            og[g] = (to_col(gts[g, s : s + 1, :]) * grads[g].astype(F32)).astype(BF16)

        pre[0:n] = dot(rows[...].reshape(m, 1024), w[...], 1, 0).reshape(n, CAP, 768)
        act[0:n] = dot(og[0:n].reshape(m, 1024), wd[...], 1, 1).reshape(n, CAP, 384)

        @pl.loop(0, n)
        def _(g):
            pg, pu, ag = pre[g, :, 0:384], pre[g, :, 384:768], act[g]
            sigma = lax.logistic(pg)
            ac[g] = (pg * sigma * pu).astype(BF16)
            gu[g, :, 0:384] = (ag * pu * sigma * (1.0 + pg * (1.0 - sigma))).astype(BF16)
            gu[g, :, 384:768] = (ag * pg * sigma).astype(BF16)

    def expert_parts(n, rows, a, d):
        m = n * CAP
        a[...] = dot(rows[...].reshape(m, 1024), gu[0:n].reshape(m, 768), 0, 0).astype(BF16).reshape(a.shape)
        spread = dot(ac[0:n].reshape(m, 384), sel[...], 1, 0).astype(BF16)
        d[...] = dot(spread, og[0:n].reshape(m, 1024), 0, 0).astype(BF16).reshape(d.shape)

    def expert_gates(n, grads, s, wd):
        m = n * CAP
        made[0:n] = dot(ac[0:n].reshape(m, 384), wd[...], 1, 0).reshape(n, CAP, 1024)

        @pl.loop(0, n)
        def _(g):
            col = jnp.sum(grads[g].astype(F32) * made[g], axis=1, keepdims=True)
            gg[g, s] = to_row(col.astype(BF16).astype(F32))

    def expert_back(n, w, back):
        m = n * CAP
        back[...] = dot(gu[0:n].reshape(m, 768), w[...], 1, 1).astype(BF16).reshape(back.shape)

    def give_gates(s, n):
        return [
            remote(gg.at[i, s], gg_in.at[i, s], gg_send.at[s, i], gg_recv.at[s, i], z=wrap(z - DIST[i] + NZ, NZ))
            for i in ORDER
            if i < n
        ]

    def give_rows(back, n, base):
        return [
            remote(back.at[i], rows_in.at[base + i], row_send.at[base + i], row_recv.at[base + i], z=wrap(z - DIST[i] + NZ, NZ))
            for i in ORDER
            if i < n
        ]

    def swap_core(a, d, a_in, d_in, e):
        return [
            remote(a.at[:, other], a_in, sib_send.at[e, 0], sib_recv.at[e, 0], c=other),
            remote(d.at[:, other], d_in, sib_send.at[e, 1], sib_recv.at[e, 1], c=other),
        ]

    def add_core(a, d, a_in, d_in, s_a, s_d):
        @pl.loop(0, NCHIP)
        def _(k):
            s_a[k] = (a[k, c].astype(F32) + a_in[k].astype(F32)).astype(BF16)
            s_d[k] = (d[k, c].astype(F32) + d_in[k].astype(F32)).astype(BF16)

    def scatter(e, k, s_a, s_d, rb_a, rb_d):
        to, where = chip(k)
        return [
            remote(s_a.at[to], rb_a.at[me], rs_send.at[e, 0, k], rs_recv.at[e, 0, k], **where),
            remote(s_d.at[to], rb_d.at[me], rs_send.at[e, 1, k], rs_recv.at[e, 1, k], **where),
        ]

    def scattered(e, k, s_a, s_d, rb_a, rb_d):
        frm, where = chip_from(k)
        return [
            remote(s_a.at[0], rb_a.at[frm], rs_send.at[e, 0, k], rs_recv.at[e, 0, k], **where),
            remote(s_d.at[0], rb_d.at[frm], rs_send.at[e, 1, k], rs_recv.at[e, 1, k], **where),
        ]

    for m in range(2):
        half(m, other).wait_recv()
    for cp in first:
        cp.wait_recv()
    expert_rows(NS, stok, sgrad, 1, w2, w2d)
    expert_parts(NS, stok, sa, sd)
    swap_s = swap_core(sa, sd, sib_sa, sib_sd, 1)
    starts(swap_s)
    expert_gates(NS, sgrad, 1, w2d)
    gates_s = give_gates(1, NS)
    starts(gates_s)
    expert_back(NS, w2, srow)
    rows_s = give_rows(srow, NS, NP)
    starts(rows_s)
    rows_in[NP + HOME] = srow[HOME]
    gg_in[HOME, 1] = gg[HOME, 1]
    for cp in swap_s:
        cp.wait_recv()
    add_core(sa, sd, sib_sa, sib_sd, s_sa, s_sd)
    arrays_s = (s_sa, s_sd, rb_sa, rb_sd)

    @pl.loop(1, NCHIP)
    def _(k):
        starts(scatter(1, k, *arrays_s))

    rb_sa[me] = s_sa[me]
    rb_sd[me] = s_sd[me]

    for cp in later:
        cp.wait_recv()
    expert_rows(NP, ptok, pgrad, 0, w1, w1d)
    expert_gates(NP, pgrad, 0, w1d)
    gates_p = give_gates(0, NP)
    starts(gates_p)
    expert_parts(NP, ptok, pa, pd)
    swap_p = swap_core(pa, pd, sib_pa, sib_pd, 0)
    starts(swap_p)
    expert_back(NP, w1, prow)
    rows_p = give_rows(prow, NP, 0)
    starts(rows_p)
    rows_in[HOME] = prow[HOME]
    gg_in[HOME, 0] = gg[HOME, 0]

    for cp in gates_p + gates_s:
        cp.wait_recv()
    for g in range(16):
        i, s = (g, 0) if g < NP else (g - NP, 1)
        col = to_col(gg_in[i, s])
        vbuf[g * CAP : (g + 1) * CAP, :] = jnp.where(lane == expert_of(g), col, 0.0).astype(BF16)
    grads = dot(oh[...], vbuf[...], 0, 0)
    p = prob[...]
    logit_grad = (p * (grads - jnp.sum(p * grads, axis=1, keepdims=True))).astype(BF16)
    part[...] = dot(tok[...], logit_grad, 0, 0).astype(BF16).reshape(part.shape)

    def r2(k):
        to, where = plane(k)
        return remote(part.at[to], r_in.at[mine32], r2_send.at[k], r2_recv.at[k], **where)

    def r2_from(k):
        frm, where = plane_back(k)
        return remote(part.at[0], r_in.at[frm], r2_send.at[k], r2_recv.at[k], **where)

    @pl.loop(1, NDP)
    def _(k):
        r2(k).start()

    r_in[mine32] = part[mine32]
    for cp in swap_p:
        cp.wait_recv()
    add_core(pa, pd, sib_pa, sib_pd, s_pa, s_pd)
    arrays_p = (s_pa, s_pd, rb_pa, rb_pd)

    @pl.loop(1, NCHIP)
    def _(k):
        starts(scatter(0, k, *arrays_p))

    rb_pa[me] = s_pa[me]
    rb_pd[me] = s_pd[me]

    @pl.loop(1, NCHIP)
    def _(k):
        for cp in scattered(1, k, *arrays_s):
            cp.wait_recv()

    za_out[...] = jnp.sum(rb_sa[...].astype(F32), axis=0).astype(BF16)
    zd_out[...] = jnp.sum(rb_sd[...].astype(F32), axis=0).astype(BF16)

    @pl.loop(1, NDP)
    def _(k):
        r2_from(k).wait_recv()

    r_zin[z] = jnp.sum(r_in[...].astype(F32), axis=0).astype(BF16)

    def r3(k):
        return remote(r_zin.at[z], r_zin.at[z], r3_send.at[k], r3_recv.at[k], z=wrap(z + k, NZ))

    def r3_from(k):
        frm = wrap(z - k + NZ, NZ)
        return remote(r_zin.at[frm], r_zin.at[frm], r3_send.at[k], r3_recv.at[k], z=frm)

    @pl.loop(1, NZ)
    def _(k):
        r3(k).start()

    zs = [
        remote(za_out, za_in, zs_sem.at[0], zs_sem.at[1], z=far),
        remote(zd_out, zd_in, zs_sem.at[2], zs_sem.at[3], z=far),
    ]
    starts(zs)

    for cp in rows_p + rows_s:
        cp.wait_recv()
    out_tok[...] = (
        dot(oh[...], rows_in[...].reshape(512, 1024), 0, 0) + dot(logit_grad, rw[...], 1, 1)
    ).astype(BF16)

    @pl.loop(1, NZ)
    def _(k):
        r3_from(k).wait_recv()

    r_out[mine32] = jnp.sum(r_zin[...].astype(F32), axis=0).astype(BF16)

    def r5(k):
        ref = r_out.at[mine32]
        return remote(ref, ref, r5_send.at[k], r5_recv.at[k], **plane(k)[1])

    def r5_from(k):
        frm, where = plane_back(k)
        ref = r_out.at[frm]
        return remote(ref, ref, r5_send.at[k], r5_recv.at[k], **where)

    @pl.loop(1, NDP)
    def _(k):
        r5(k).start()

    @pl.loop(1, NCHIP)
    def _(k):
        for cp in scattered(0, k, *arrays_p):
            cp.wait_recv()

    total = jnp.sum(rb_pa[...].astype(F32), axis=0)
    out_g[...] = total[:, :384]
    out_u[...] = total[:, 384:]
    total_d[...] = jnp.sum(rb_pd[...].astype(F32), axis=0)

    for cp in to_far + first + later + swap_p + swap_s + gates_p + gates_s + rows_p + rows_s:
        cp.wait_send()
    for m in range(2):
        half(m, c).wait_send()

    @pl.loop(1, NCHIP)
    def _(k):
        for m in range(2):
            plane_copy(m, k).wait_send()
        for cp in scatter(0, k, *arrays_p) + scatter(1, k, *arrays_s):
            cp.wait_send()
        r3(k).wait_send()

    @pl.loop(1, NDP)
    def _(k):
        r2(k).wait_send()
        r5(k).wait_send()

    for cp in zs:
        cp.wait()
    out_g[...] += za_in[:, :384].astype(F32)
    out_u[...] += za_in[:, 384:].astype(F32)
    total_d[...] += zd_in[...].astype(F32)
    for n in range(8):
        out_d[:, n, :] = total_d[0:12, n * 128 : (n + 1) * 128]

    @pl.loop(1, NDP)
    def _(k):
        r5_from(k).wait_recv()

    out_r[...] = r_out[...].reshape(1024, 128).astype(F32)


def local(tokens, grad_out, expert_ids, router_weight, wg, wu, wd):
    hbm = pl.BlockSpec(memory_space=pl.ANY)
    vmem = pl.BlockSpec(memory_space=pltpu.VMEM)
    dma = pltpu.SemaphoreType.DMA
    V = pltpu.VMEM
    blocks = [V((NCHIP, 32, 768), BF16), V((NCHIP, 16, 1024), BF16)]
    grad_tokens, gate, up, down, router = pl.pallas_call(
        whole,
        out_shape=(
            jax.ShapeDtypeStruct((256, 1024), BF16),
            jax.ShapeDtypeStruct((32, 384), F32),
            jax.ShapeDtypeStruct((32, 384), F32),
            jax.ShapeDtypeStruct((12, 8, 128), F32),
            jax.ShapeDtypeStruct((1024, 128), F32),
        ),
        in_specs=[hbm] * 7,
        out_specs=(vmem,) * 5,
        scratch_shapes=[
            V((256, 1024), BF16), V((256, 1024), BF16), V((8, 256), jnp.int32), V((1024, 128), BF16),
            V((1024, 768), BF16), V((384, 1024), BF16), V((1024, 768), BF16), V((384, 1024), BF16),
            V((512, 256), BF16), V((256, 128), F32), V((16, CAP, 1024), BF16), V((16, CAP, 1024), BF16),
            V((NP, 8, 128), F32), V((384, 512), BF16),
            V((NP, CAP, 1024), BF16), V((NS, CAP, 1024), BF16), V((NP, CAP, 1024), BF16), V((NS, CAP, 1024), BF16),
            V((NP, 8, 128), F32),
            V((NP, CAP, 768), F32), V((NP, CAP, 384), F32), V((NP, CAP, 1024), BF16),
            V((NP, CAP, 768), BF16), V((NP, CAP, 384), BF16), V((NP, CAP, 1024), F32),
            V((NP, CAP, 1024), BF16), V((NS, CAP, 1024), BF16), V((NP, 2, 1, 128), F32),
            V((16, CAP, 1024), BF16), V((NP, 2, 1, 128), F32), V((512, 128), BF16),
            V((16, 2, 32, 768), BF16), V((16, 2, 16, 1024), BF16),
            V((16, 2, 32, 768), BF16), V((16, 2, 16, 1024), BF16),
            *blocks, *blocks, *blocks, *blocks, *blocks, *blocks,
            V((32, 768), BF16), V((16, 1024), BF16), V((32, 768), BF16), V((16, 1024), BF16),
            V((16, 1024), F32), V((NDP, 32, 128), BF16), V((NDP, 32, 128), BF16),
            V((NZ, 32, 128), BF16), V((NDP, 32, 128), BF16),
            dma((7,)), dma((16,)), dma((16,)), dma((16,)), dma((16,)), dma((9,)), dma((9,)),
            dma((2,)), dma((2,)), dma((2, 16)), dma((2, 16)), dma((2,)), dma((2,)),
            dma((16,)), dma((16,)), dma((2, 9)), dma((2, 9)),
            dma((2, 2)), dma((2, 2)), dma((2, 2, 16)), dma((2, 2, 16)), dma((4,)),
            dma((NDP,)), dma((NDP,)), dma((16,)), dma((16,)), dma((NDP,)), dma((NDP,)),
        ],
        compiler_params=pltpu.CompilerParams(
            collective_id=0, has_side_effects=True, vmem_limit_bytes=52 << 20
        ),
        name="whole",
    )(tokens, grad_out, expert_ids.T, router_weight, wg[0], wu[0], wd[0])
    return (
        grad_tokens,
        gate[None],
        up[None],
        down.reshape(1, 12, 1024),
        router,
    )


def solution(mesh):
    finer = Mesh(mesh.devices.reshape(4, 4, 2, NZ), AX)
    dp = AX[:3]
    return jax.shard_map(
        local,
        mesh=finer,
        in_specs=(
            P(AX, None), P(AX, None), P(AX, None), P(),
            P("expert", None, None), P("expert", None, None), P("expert", None, None),
        ),
        out_specs=(
            P(AX, None), P("expert", dp, None), P("expert", dp, None), P("expert", dp, None), P(),
        ),
        check_vma=False,
    )
```

```python
import jax
import jax.numpy as jnp
from jax import lax
from jax.experimental import pallas as pl
from jax.experimental.pallas import tpu as pltpu
from jax.sharding import Mesh
from jax.sharding import PartitionSpec as P

AX = ("dp_0", "dp_1", "dp_2", "expert")
MESH = pl.DeviceIdType.MESH
F32, BF16 = jnp.float32, jnp.bfloat16

NZ = 16
NCHIP = 16
CAP = 32
DIST = (-3, -2, -1, 0, 1, 2, 3, 4, -4)
RELATIVE = tuple(d % NZ for d in DIST) + tuple((d + 8) % NZ for d in DIST[:7])
NP, NS = 9, 7
HOME = 3
ORDER = (7, 8, 0, 6, 1, 5, 2, 4)
NDP = 32


def wrap(v, n):
    return lax.rem(v + n, n)


def at(where):
    return {AX["xycz".index(k)]: v for k, v in where.items()}


def remote(src, dst, send, recv, **where):
    return pltpu.make_async_remote_copy(
        src_ref=src, dst_ref=dst, send_sem=send, recv_sem=recv, device_id=at(where), device_id_type=MESH
    )


def dot(a, b, ca, cb):
    return lax.dot_general(a, b, (((ca,), (cb,)), ((), ())), preferred_element_type=F32)


def starts(copies):
    for cp in copies:
        cp.start()


def whole(
    tok_h, grad_h, ids_h, rw_h, wg_h, wu_h, wd_h,
    out_tok, out_g, out_u, out_d, out_r,
    tok, grad, ids, rw, w1, w1d, w2, w2d,
    oh, prob, st, sg, sgt, sel,
    ptok, stok, pgrad, sgrad, gts,
    pre, act, og, gu, ac, made,
    prow, srow, gg, rows_in, gg_in, vbuf,
    pa, pd, sa, sd, sib_pa, sib_pd, sib_sa, sib_sd,
    s_pa, s_pd, s_sa, s_sd, rb_pa, rb_pd, rb_sa, rb_sd,
    za_out, zd_out, za_in, zd_in,
    total_d, part, r_in, r_zin, r_out,
    loc, row_sem, gt_sem,
    wz_send, wz_recv, wp_send, wp_recv, wc_send, wc_recv,
    back_send, back_recv, gg_send, gg_recv,
    sib_send, sib_recv, rs_send, rs_recv, zs_sem,
    r_sem,
):
    x, y, c, z = tuple(lax.axis_index(a) for a in AX)
    me = x * 4 + y
    other = 1 - c
    far = wrap(z + 8, NZ)

    fetch = [
        pltpu.make_async_copy(ids_h, ids, loc.at[0]),
        pltpu.make_async_copy(tok_h, tok, loc.at[1]),
        pltpu.make_async_copy(rw_h, rw, loc.at[2]),
        pltpu.make_async_copy(grad_h, grad, loc.at[3]),
        pltpu.make_async_copy(wg_h, w1.at[:, pl.ds(0, 384)], loc.at[4]),
        pltpu.make_async_copy(wu_h, w1.at[:, pl.ds(384, 384)], loc.at[5]),
        pltpu.make_async_copy(wd_h, w1d, loc.at[6]),
    ]
    starts(fetch)

    barrier = pltpu.get_barrier_semaphore()
    mine32 = me * 2 + c

    def plane(k):
        to = wrap(mine32 + k, NDP)
        return to, dict(x=to // 8, y=lax.rem(to // 2, 4), c=lax.rem(to, 2))

    def plane_back(k):
        frm = wrap(mine32 - k + NDP, NDP)
        return frm, dict(x=frm // 8, y=lax.rem(frm // 2, 4), c=lax.rem(frm, 2))

    partners = [dict(z=wrap(z + d, NZ)) for d in range(1, NZ)] + [plane(k)[1] for k in range(1, NDP)]
    for where in partners:
        pl.semaphore_signal(barrier, inc=1, device_id=at(where), device_id_type=MESH)

    def chip(k):
        to = wrap(me + k, NCHIP)
        return to, dict(x=to // 4, y=lax.rem(to, 4))

    def chip_from(k):
        frm = wrap(me - k + NCHIP, NCHIP)
        return frm, dict(x=frm // 4, y=lax.rem(frm, 4))

    lane = lax.broadcasted_iota(jnp.int32, (CAP, 128), 1)
    sub = lax.broadcasted_iota(jnp.int32, (CAP, 128), 0)

    def expert_of(g):
        return 8 * lax.rem(z + RELATIVE[g], NZ)

    def to_row(col):
        return jnp.sum(jnp.where(lane == sub, col, 0.0), axis=0, keepdims=True)

    def to_col(row):
        return jnp.sum(jnp.where(lane == sub, row, 0.0), axis=1, keepdims=True)

    fetch[0].wait()
    every = lax.broadcasted_iota(jnp.int32, (128, 256), 0)
    names = ids[0:1, :] == every
    for k in range(1, 8):
        names = jnp.logical_or(names, ids[k : k + 1, :] == every)
    mask = jnp.where(names, 1.0, 0.0).astype(BF16)
    unit = lax.broadcasted_iota(jnp.int32, (128, 128), 0) == lax.broadcasted_iota(jnp.int32, (128, 128), 1)
    named = dot(mask, jnp.where(unit, 1.0, 0.0).astype(BF16), 0, 0) > 0.5
    row16 = lax.broadcasted_iota(jnp.int32, (16, 128), 0)
    rel = jnp.zeros((16, 128), jnp.int32)
    for g in range(16):
        rel = jnp.where(row16 == g, expert_of(g), rel)
    mine = jnp.where(lax.broadcasted_iota(jnp.int32, (16, 128), 1) == rel, 1.0, 0.0).astype(BF16)
    served = dot(mine, mask, 1, 0)
    before = lax.broadcasted_iota(jnp.int32, (256, 256), 0) < lax.broadcasted_iota(jnp.int32, (256, 256), 1)
    rank = dot(served.astype(BF16), jnp.where(before, 1.0, 0.0).astype(BF16), 1, 0)
    slot = jnp.where(served > 0.5, rank, -1.0)
    want = lax.broadcasted_iota(jnp.int32, (CAP, 256), 0).astype(F32)
    for g in range(16):
        oh[g * CAP : (g + 1) * CAP, :] = jnp.where(slot[g : g + 1, :] == want, 1.0, 0.0).astype(BF16)
    fetch[1].wait()
    st[...] = dot(oh[...], tok[...], 1, 0).astype(BF16).reshape(st.shape)
    fetch[2].wait()
    logits = dot(tok[...], rw[...], 1, 0)
    raised = jnp.where(named, jnp.exp(logits), 0.0)
    prob[...] = raised / jnp.sum(raised, axis=1, keepdims=True)
    slot_prob = dot(oh[...], prob[...].astype(BF16), 1, 0)
    sgt[...] = jnp.zeros_like(sgt)
    for g in range(16):
        i, s = (g, 0) if g < NP else (g - NP, 1)
        col = jnp.sum(
            jnp.where(lane == expert_of(g), slot_prob[g * CAP : (g + 1) * CAP, :], 0.0), axis=1, keepdims=True
        )
        sgt[i, s : s + 1, :] = to_row(col)
    fetch[3].wait()
    sg[...] = dot(oh[...], grad[...], 1, 0).astype(BF16).reshape(sg.shape)
    for cp in fetch[4:]:
        cp.wait()

    pl.semaphore_wait(barrier, len(partners))

    def piece(ref, m, core, p):
        if m == 0:
            return ref.at[pl.ds(pl.multiple_of(512 * core + 32 * p, 32), 32)]
        row = pl.multiple_of(192 * core + 48 * (p // 4), 16)
        col = pl.multiple_of(256 * lax.rem(p, 4), 128)
        return ref.at[pl.ds(row, 48), pl.ds(col, 256)]

    own, second = (w1, w1d), (w2, w2d)
    to_far = [
        remote(piece(own[m], m, c, me), piece(second[m], m, c, me), wz_send.at[m], wz_recv.at[m], z=far)
        for m in range(2)
    ]
    starts(to_far)

    first, later = [], []
    for i in ORDER:
        to = wrap(z + DIST[i], NZ)
        first.append(remote(sgt.at[i], gts.at[i], gt_sem.at[0], gt_sem.at[1], z=to))
        later.append(remote(st.at[i], ptok.at[i], row_sem.at[0], row_sem.at[1], z=to))
        later.append(remote(sg.at[i], pgrad.at[i], row_sem.at[2], row_sem.at[3], z=to))
        if i < NS:
            j = NP + i
            first.append(remote(st.at[j], stok.at[i], row_sem.at[4], row_sem.at[5], z=to))
            first.append(remote(sg.at[j], sgrad.at[i], row_sem.at[6], row_sem.at[7], z=to))
    starts(first)
    starts(later)

    def group(ref, n, send, recv):
        refs = ref.at[pl.ds(0, n)]
        return remote(refs, refs, send, recv, z=far)

    gt_all = group(gts, NP - 1, gt_sem.at[0], gt_sem.at[1])
    first_all = [
        group(stok, NS - 1, row_sem.at[4], row_sem.at[5]),
        group(sgrad, NS - 1, row_sem.at[6], row_sem.at[7]),
        gt_all,
    ]
    later_all = [
        group(ptok, NP - 1, row_sem.at[0], row_sem.at[1]),
        group(pgrad, NP - 1, row_sem.at[2], row_sem.at[3]),
    ]
    gts[HOME] = sgt[HOME]
    ptok[HOME] = st[HOME]
    pgrad[HOME] = sg[HOME]
    stok[HOME] = st[NP + HOME]
    sgrad[HOME] = sg[NP + HOME]

    q = lax.broadcasted_iota(jnp.int32, (384, 512), 1)
    unit = lax.broadcasted_iota(jnp.int32, (384, 512), 0)
    block, k16 = q // 16, lax.rem(q, 16)
    sel[...] = jnp.where(jnp.logical_and(unit == block * 12 + k16, k16 < 12), 1.0, 0.0).astype(BF16)

    for cp in to_far:
        cp.wait_recv()

    def plane_copy(m, k):
        _to, where = chip(k)
        mine_ = piece(second[m], m, c, me)
        return remote(mine_, mine_, wp_send.at[m], wp_recv.at[m], **where)

    plane_all = [
        remote(ref, ref, wp_send.at[m], wp_recv.at[m], c=other)
        for m, ref in enumerate((w2.at[pl.ds(0, 480)], w2d.at[pl.ds(0, 240), pl.ds(0, 768)]))
    ]

    @pl.loop(1, NCHIP)
    def _(k):
        for m in range(2):
            plane_copy(m, k).start()

    for cp in plane_all:
        cp.wait_recv()

    def half(m, core):
        n = 512 if m == 0 else 192
        ref = second[m].at[pl.ds(pl.multiple_of(n * core, n), n)]
        return remote(ref, ref, wc_send.at[m], wc_recv.at[m], c=other)

    for m in range(2):
        half(m, c).start()

    def expert_rows(n, rows, grads, s, w, wd):
        m = n * CAP

        @pl.loop(0, n)
        def _(g):
            og[g] = (to_col(gts[g, s : s + 1, :]) * grads[g].astype(F32)).astype(BF16)

        pre[0:n] = dot(rows[...].reshape(m, 1024), w[...], 1, 0).reshape(n, CAP, 768)
        act[0:n] = dot(og[0:n].reshape(m, 1024), wd[...], 1, 1).reshape(n, CAP, 384)

        @pl.loop(0, n)
        def _(g):
            pg, pu, ag = pre[g, :, 0:384], pre[g, :, 384:768], act[g]
            sigma = lax.logistic(pg)
            ac[g] = (pg * sigma * pu).astype(BF16)
            gu[g, :, 0:384] = (ag * pu * sigma * (1.0 + pg * (1.0 - sigma))).astype(BF16)
            gu[g, :, 384:768] = (ag * pg * sigma).astype(BF16)

    def expert_parts(n, rows, a, d):
        m = n * CAP
        a[...] = dot(rows[...].reshape(m, 1024), gu[0:n].reshape(m, 768), 0, 0).astype(BF16).reshape(a.shape)
        spread = dot(ac[0:n].reshape(m, 384), sel[...], 1, 0).astype(BF16)
        d[...] = dot(spread, og[0:n].reshape(m, 1024), 0, 0).astype(BF16).reshape(d.shape)

    def expert_gates(n, grads, s, wd):
        m = n * CAP
        made[0:n] = dot(ac[0:n].reshape(m, 384), wd[...], 1, 0).reshape(n, CAP, 1024)

        @pl.loop(0, n)
        def _(g):
            col = jnp.sum(grads[g].astype(F32) * made[g], axis=1, keepdims=True)
            gg[g, s] = to_row(col.astype(BF16).astype(F32))

    def expert_back(n, w, back):
        m = n * CAP
        back[...] = dot(gu[0:n].reshape(m, 768), w[...], 1, 1).astype(BF16).reshape(back.shape)

    def give_gates(s, n):
        return [
            remote(gg.at[i, s], gg_in.at[i, s], gg_send.at[s], gg_recv.at[s], z=wrap(z - DIST[i] + NZ, NZ))
            for i in ORDER
            if i < n
        ]

    def give_rows(back, n, base):
        return [
            remote(back.at[i], rows_in.at[base + i], back_send.at[base // NP], back_recv.at[base // NP], z=wrap(z - DIST[i] + NZ, NZ))
            for i in ORDER
            if i < n
        ]

    def swap_core(a, d, a_in, d_in, e):
        return [
            remote(a.at[:, other], a_in, sib_send.at[e, 0], sib_recv.at[e, 0], c=other),
            remote(d.at[:, other], d_in, sib_send.at[e, 1], sib_recv.at[e, 1], c=other),
        ]

    def add_core(a, d, a_in, d_in, s_a, s_d):
        @pl.loop(0, NCHIP)
        def _(k):
            s_a[k] = (a[k, c].astype(F32) + a_in[k].astype(F32)).astype(BF16)
            s_d[k] = (d[k, c].astype(F32) + d_in[k].astype(F32)).astype(BF16)

    def scatter(e, k, s_a, s_d, rb_a, rb_d):
        to, where = chip(k)
        return [
            remote(s_a.at[to], rb_a.at[me], rs_send.at[e, 0], rs_recv.at[e, 0], **where),
            remote(s_d.at[to], rb_d.at[me], rs_send.at[e, 1], rs_recv.at[e, 1], **where),
        ]

    def scattered_all(e, rb_a, rb_d):
        return [
            group(rb_a, NCHIP - 1, rs_send.at[e, 0], rs_recv.at[e, 0]),
            group(rb_d, NCHIP - 1, rs_send.at[e, 1], rs_recv.at[e, 1]),
        ]

    for m in range(2):
        half(m, other).wait_recv()
    for cp in first_all:
        cp.wait_recv()
    expert_rows(NS, stok, sgrad, 1, w2, w2d)
    expert_parts(NS, stok, sa, sd)
    swap_s = swap_core(sa, sd, sib_sa, sib_sd, 1)
    starts(swap_s)
    expert_gates(NS, sgrad, 1, w2d)
    gates_s = give_gates(1, NS)
    starts(gates_s)
    expert_back(NS, w2, srow)
    rows_s = give_rows(srow, NS, NP)
    starts(rows_s)
    rows_in[NP + HOME] = srow[HOME]
    gg_in[HOME, 1] = gg[HOME, 1]
    for cp in swap_s:
        cp.wait_recv()
    add_core(sa, sd, sib_sa, sib_sd, s_sa, s_sd)
    arrays_s = (s_sa, s_sd, rb_sa, rb_sd)

    @pl.loop(1, NCHIP)
    def _(k):
        starts(scatter(1, k, *arrays_s))

    rb_sa[me] = s_sa[me]
    rb_sd[me] = s_sd[me]

    for cp in scattered_all(1, rb_sa, rb_sd):
        cp.wait_recv()
    za_out[...] = jnp.sum(rb_sa[...].astype(F32), axis=0).astype(BF16)
    zd_out[...] = jnp.sum(rb_sd[...].astype(F32), axis=0).astype(BF16)
    for cp in later_all:
        cp.wait_recv()
    expert_rows(NP, ptok, pgrad, 0, w1, w1d)
    expert_gates(NP, pgrad, 0, w1d)
    gates_p = give_gates(0, NP)
    starts(gates_p)
    zs = [
        remote(za_out, za_in, zs_sem.at[0], zs_sem.at[1], z=far),
        remote(zd_out, zd_in, zs_sem.at[2], zs_sem.at[3], z=far),
    ]
    starts(zs)
    expert_parts(NP, ptok, pa, pd)
    swap_p = swap_core(pa, pd, sib_pa, sib_pd, 0)
    starts(swap_p)
    expert_back(NP, w1, prow)
    rows_p = give_rows(prow, NP, 0)
    starts(rows_p)
    rows_in[HOME] = prow[HOME]
    gg_in[HOME, 0] = gg[HOME, 0]

    gates_all = [group(gg_in.at[:, s], n - 1, gg_send.at[s], gg_recv.at[s]) for s, n in enumerate((NP, NS))]
    for cp in gates_all:
        cp.wait_recv()
    for g in range(16):
        i, s = (g, 0) if g < NP else (g - NP, 1)
        col = to_col(gg_in[i, s])
        vbuf[g * CAP : (g + 1) * CAP, :] = jnp.where(lane == expert_of(g), col, 0.0).astype(BF16)
    grads = dot(oh[...], vbuf[...], 0, 0)
    p = prob[...]
    logit_grad = (p * (grads - jnp.sum(p * grads, axis=1, keepdims=True))).astype(BF16)
    part[...] = dot(tok[...], logit_grad, 0, 0).astype(BF16).reshape(part.shape)

    def r2(k):
        to, where = plane(k)
        return remote(part.at[to], r_in.at[mine32], r_sem.at[2, 0], r_sem.at[2, 1], **where)

    r2_all = group(r_in, NDP - 1, r_sem.at[2, 0], r_sem.at[2, 1])

    @pl.loop(1, NDP)
    def _(k):
        r2(k).start()

    r_in[mine32] = part[mine32]
    for cp in swap_p:
        cp.wait_recv()
    add_core(pa, pd, sib_pa, sib_pd, s_pa, s_pd)
    arrays_p = (s_pa, s_pd, rb_pa, rb_pd)

    @pl.loop(1, NCHIP)
    def _(k):
        starts(scatter(0, k, *arrays_p))

    rb_pa[me] = s_pa[me]
    rb_pd[me] = s_pd[me]

    r2_all.wait_recv()

    r_zin[z] = jnp.sum(r_in[...].astype(F32), axis=0).astype(BF16)

    def r3(k):
        return remote(r_zin.at[z], r_zin.at[z], r_sem.at[3, 0], r_sem.at[3, 1], z=wrap(z + k, NZ))

    r3_all = group(r_zin, NZ - 1, r_sem.at[3, 0], r_sem.at[3, 1])

    @pl.loop(1, NZ)
    def _(k):
        r3(k).start()

    rows_all = [group(rows_in, n - 1, back_send.at[e], back_recv.at[e]) for e, n in enumerate((NP, NS))]
    for cp in rows_all:
        cp.wait_recv()
    out_tok[...] = (
        dot(oh[...], rows_in[...].reshape(512, 1024), 0, 0) + dot(logit_grad, rw[...], 1, 1)
    ).astype(BF16)

    r3_all.wait_recv()

    r_out[mine32] = jnp.sum(r_zin[...].astype(F32), axis=0).astype(BF16)

    def r5(k):
        ref = r_out.at[mine32]
        return remote(ref, ref, r_sem.at[5, 0], r_sem.at[5, 1], **plane(k)[1])

    r5_all = group(r_out, NDP - 1, r_sem.at[5, 0], r_sem.at[5, 1])

    @pl.loop(1, NDP)
    def _(k):
        r5(k).start()

    for cp in scattered_all(0, rb_pa, rb_pd):
        cp.wait_recv()

    total = jnp.sum(rb_pa[...].astype(F32), axis=0)
    out_g[...] = total[:, :384]
    out_u[...] = total[:, 384:]
    total_d[...] = jnp.sum(rb_pd[...].astype(F32), axis=0)

    for cp in to_far + first_all + later_all + swap_p + swap_s + gates_all + rows_all + plane_all:
        cp.wait_send()
    for cp in scattered_all(0, rb_pa, rb_pd) + scattered_all(1, rb_sa, rb_sd) + [r2_all, r3_all, r5_all]:
        cp.wait_send()
    for m in range(2):
        half(m, c).wait_send()
    for cp in zs:
        cp.wait()
    out_g[...] += za_in[:, :384].astype(F32)
    out_u[...] += za_in[:, 384:].astype(F32)
    total_d[...] += zd_in[...].astype(F32)
    for n in range(8):
        out_d[:, n, :] = total_d[0:12, n * 128 : (n + 1) * 128]

    r5_all.wait_recv()

    out_r[...] = r_out[...].reshape(1024, 128).astype(F32)


def local(tokens, grad_out, expert_ids, router_weight, wg, wu, wd):
    hbm = pl.BlockSpec(memory_space=pltpu.HBM)
    vmem = pl.BlockSpec(memory_space=pltpu.VMEM)
    dma = pltpu.SemaphoreType.DMA
    V = pltpu.VMEM
    blocks = [V((NCHIP, 32, 768), BF16), V((NCHIP, 16, 1024), BF16)]
    grad_tokens, gate, up, down, router = pl.pallas_call(
        whole,
        out_shape=(
            jax.ShapeDtypeStruct((256, 1024), BF16),
            jax.ShapeDtypeStruct((32, 384), F32),
            jax.ShapeDtypeStruct((32, 384), F32),
            jax.ShapeDtypeStruct((12, 8, 128), F32),
            jax.ShapeDtypeStruct((1024, 128), F32),
        ),
        in_specs=[hbm] * 7,
        out_specs=(vmem,) * 5,
        scratch_shapes=[
            V((256, 1024), BF16), V((256, 1024), BF16), V((8, 256), jnp.int32), V((1024, 128), BF16),
            V((1024, 768), BF16), V((384, 1024), BF16), V((1024, 768), BF16), V((384, 1024), BF16),
            V((512, 256), BF16), V((256, 128), F32), V((16, CAP, 1024), BF16), V((16, CAP, 1024), BF16),
            V((NP, 8, 128), F32), V((384, 512), BF16),
            V((NP, CAP, 1024), BF16), V((NS, CAP, 1024), BF16), V((NP, CAP, 1024), BF16), V((NS, CAP, 1024), BF16),
            V((NP, 8, 128), F32),
            V((NP, CAP, 768), F32), V((NP, CAP, 384), F32), V((NP, CAP, 1024), BF16),
            V((NP, CAP, 768), BF16), V((NP, CAP, 384), BF16), V((NP, CAP, 1024), F32),
            V((NP, CAP, 1024), BF16), V((NS, CAP, 1024), BF16), V((NP, 2, 1, 128), F32),
            V((16, CAP, 1024), BF16), V((NP, 2, 1, 128), F32), V((512, 128), BF16),
            V((16, 2, 32, 768), BF16), V((16, 2, 16, 1024), BF16),
            V((16, 2, 32, 768), BF16), V((16, 2, 16, 1024), BF16),
            *blocks, *blocks, *blocks, *blocks, *blocks, *blocks,
            V((32, 768), BF16), V((16, 1024), BF16), V((32, 768), BF16), V((16, 1024), BF16),
            V((16, 1024), F32), V((NDP, 32, 128), BF16), V((NDP, 32, 128), BF16),
            V((NZ, 32, 128), BF16), V((NDP, 32, 128), BF16),
            dma((7,)), dma((8,)), dma((2,)),
            dma((2,)), dma((2,)), dma((2,)), dma((2,)), dma((2,)), dma((2,)),
            dma((2,)), dma((2,)), dma((2,)), dma((2,)),
            dma((2, 2)), dma((2, 2)), dma((2, 2)), dma((2, 2)), dma((4,)),
            dma((6, 2)),
        ],
        compiler_params=pltpu.CompilerParams(
            collective_id=0, has_side_effects=True, vmem_limit_bytes=52 << 20
        ),
        name="whole",
    )(*(pltpu.with_memory_space_constraint(v, pltpu.HBM) for v in (tokens, grad_out, expert_ids.T, router_weight, wg[0], wu[0], wd[0])))
    return (
        grad_tokens,
        gate[None],
        up[None],
        down.reshape(1, 12, 1024),
        router,
    )


def solution(mesh):
    finer = Mesh(mesh.devices.reshape(4, 4, 2, NZ), AX)
    dp = AX[:3]
    return jax.shard_map(
        local,
        mesh=finer,
        in_specs=(
            P(AX, None), P(AX, None), P(AX, None), P(),
            P("expert", None, None), P("expert", None, None), P("expert", None, None),
        ),
        out_specs=(
            P(AX, None), P("expert", dp, None), P("expert", dp, None), P("expert", dp, None), P(),
        ),
        check_vma=False,
    )
```
